256 devices in a mesh: row: 8 (over z_hi, core), col: 32 (over y, z_lo, x).
Axes of the slice: x: 4, y: 4, z: 8 (z_hi: 4, z_lo: 2; z = z_hi * 2 + z_lo), core: 2. Of those that a mesh axis runs over, the one named last changes fastest.
Arguments:
- tokens: bfloat16 [1024, 8192], P(None, 'row'), may hold values from -50 to 50
- norm_gain: float32 [8192], P('row'), may hold values from 0.5 to 1.5
- gate_vals: bfloat16 [4096, 28672], P('row', 'col'), may hold values from -0.09375 to 0.09375
- gate_meta: int32 [2048, 28672], P('row', 'col'), may hold values from 0 to 5
- up_vals: bfloat16 [4096, 28672], P('row', 'col'), may hold values from -0.09375 to 0.09375
- up_meta: int32 [2048, 28672], P('row', 'col'), may hold values from 0 to 5
- down_vals: bfloat16 [14336, 8192], P('col', 'row'), may hold values from -0.046875 to 0.046875
- down_meta: int32 [7168, 8192], P('col', 'row'), may hold values from 0 to 5
Outputs:
- layer_out: bfloat16 [1024, 8192], P(None, 'row')
The draws below stay inside these ranges and needn't reach their ends.
Inputs may be any that keep to these rules, and one draw needn't show every extreme that they name: `gate_meta`: codes 0 to 5 name the kept pair of a group of four as in the reference program. `up_meta`: as for gate_meta. `down_meta`: as for gate_meta.
All inputs are finite; a program needn't handle non-finite values.
Results may differ from the reference program's by a relative error of at most 0.0075.
Values may be sent and summed in bfloat16 or wider, within the bound.
A program may use at most 128 MiB of HBM per device.

```python
import math
import jax
import jax.numpy as jnp
from jax import lax

D = 8192
FF = 28672
BATCH = 1024


def draw_tokens(key, part):
    first, second, third = jax.random.split(jax.random.fold_in(key, 11), 3)
    row_scale = jnp.exp(jax.random.uniform(first, (BATCH, 1), minval=jnp.log(0.3), maxval=jnp.log(3.0)))
    ramp = jnp.arange(D, dtype=jnp.float32) / D
    col_scale = jnp.exp(ramp * jnp.log(3.0))[None, :] * jax.random.uniform(second, (1, D), minval=0.7, maxval=1.3)
    base = jnp.clip(jax.random.normal(third, (BATCH, D)), -4.0, 4.0)
    return (row_scale * col_scale * base).astype(jnp.bfloat16)


def place_ends(entries, rng, low, largest):
    place = [jax.random.randint(jax.random.fold_in(rng, axis), (), 0, length) for axis, length in enumerate(entries.shape)]
    main_axis = entries.shape.index(max(entries.shape))
    next_to = place[:main_axis] + [(place[main_axis] + 1) % entries.shape[main_axis]] + place[main_axis + 1:]
    return entries.at[tuple(place)].set(low).at[tuple(next_to)].set(largest)


def level_of(rng, shape, cuts, smallest, high):
    def one(axis_at, parts):
        draws = jax.random.uniform(jax.random.fold_in(jax.random.fold_in(rng, 6), axis_at), (parts,), jnp.float32, smallest / len(cuts), high / len(cuts))
        return jnp.repeat(jnp.exp(draws), shape[axis_at] // parts).reshape((-1,) + (1,) * (len(shape) - axis_at - 1))

    loudness = one(*cuts[0])
    for cut in cuts[1:]:
        loudness = loudness * one(*cut)
    return loudness


def centred(key, shape, deviation, bound, cuts=(), kind=jnp.bfloat16):
    result = deviation * jax.random.normal(key, shape, jnp.float32)
    if cuts:
        result = result * level_of(key, shape, cuts, -0.22, 0.18)
    return jnp.clip(result, -bound, bound).astype(kind)


def setup_inputs(seed: int = 0) -> dict:
    seeds = jax.random.split(jax.random.key(seed), 9)
    return {
        "tokens": draw_tokens(jax.random.fold_in(seeds[8], 71), 0),
        "norm_gain": jnp.clip(0.5 + 1.0 * jax.random.uniform(seeds[1], (D,), jnp.float32) ** level_of(seeds[1], (D,), ((0, 8),), -0.2, 0.2), 0.5, 1.5),
        "gate_vals": centred(seeds[2], (D // 2, FF), (D // 2) ** -0.5, 0.09375, ((0, 8), (1, 32))),
        "gate_meta": place_ends(jax.random.randint(seeds[3], (D // 4, FF), 0, 6), jax.random.fold_in(seeds[3], 1), 0, 5).astype(jnp.int32),
        "up_vals": centred(seeds[4], (D // 2, FF), (D // 2) ** -0.5, 0.09375, ((0, 8), (1, 32))),
        "up_meta": place_ends(jax.random.randint(seeds[5], (D // 4, FF), 0, 6), jax.random.fold_in(seeds[5], 1), 0, 5).astype(jnp.int32),
        "down_vals": centred(seeds[6], (FF // 2, D), (FF // 2) ** -0.5, 0.046875, ((0, 32), (1, 8))),
        "down_meta": place_ends(jax.random.randint(seeds[7], (FF // 4, D), 0, 6), jax.random.fold_in(seeds[7], 1), 0, 5).astype(jnp.int32),
    }


EPS = 1e-05

def expand(vals, meta):
    groups, cols = meta.shape
    first = jnp.where(meta < 3, 0, jnp.where(meta < 5, 1, 2))
    second = jnp.where(meta == 0, 1, jnp.where((meta == 1) | (meta == 3), 2, 3))
    pairs = vals.reshape(groups, 2, cols)
    leading = pairs[:, 0, :][:, None, :]
    trailing = pairs[:, 1, :][:, None, :]
    slots = jnp.arange(4, dtype=jnp.int32)[None, :, None]
    nothing = jnp.zeros((), vals.dtype)
    dense = jnp.where(first[:, None, :] == slots, leading, jnp.where(second[:, None, :] == slots, trailing, nothing))
    return dense.reshape(groups * 4, cols)

def reference(tokens, norm_gain, gate_vals, gate_meta, up_vals, up_meta, down_vals, down_meta):
    wide = tokens.astype(jnp.float32)
    scale = lax.rsqrt(lax.optimization_barrier(jnp.sum(wide * wide, axis=1, keepdims=True)) / D + EPS)
    normed = (wide * scale * norm_gain[None, :]).astype(jnp.bfloat16)
    block = math.gcd(FF, 1024)
    count = FF // block

    def step(index, total):
        start = (index * block).astype(jnp.int32)
        quarter = (index * (block // 4)).astype(jnp.int32)
        half = (index * (block // 2)).astype(jnp.int32)
        w_gate = expand(lax.dynamic_slice_in_dim(gate_vals, start, block, 1), lax.dynamic_slice_in_dim(gate_meta, start, block, 1))
        w_up = expand(lax.dynamic_slice_in_dim(up_vals, start, block, 1), lax.dynamic_slice_in_dim(up_meta, start, block, 1))
        w_down = expand(lax.dynamic_slice_in_dim(down_vals, half, block // 2, 0), lax.dynamic_slice_in_dim(down_meta, quarter, block // 4, 0))
        gate = jnp.dot(normed, w_gate, preferred_element_type=jnp.float32)
        up_part = jnp.dot(normed, w_up, preferred_element_type=jnp.float32)
        hidden = (jax.nn.silu(gate) * up_part).astype(jnp.bfloat16)
        return total + jnp.dot(hidden, w_down, preferred_element_type=jnp.float32)
    down = lax.fori_loop(0, count, step, jnp.zeros((tokens.shape[0], D), jnp.float32))
    return (wide + down).astype(jnp.bfloat16)
```

```python
import functools

import jax
import jax.numpy as jnp
from jax import lax
from jax.experimental import pallas as pl
from jax.experimental.pallas import tpu as pltpu
from jax.sharding import PartitionSpec as P

EPS = 1e-05
MESH = pl.DeviceIdType.MESH
F32 = jnp.float32
BF16 = jnp.bfloat16

CHUNKS = 8
ROWS = 128
PIECE = 16

PAIR_IN, Z_FIRST, Z_SECOND, Z_BACK, Z_LAST, PAIR_OUT = range(6)
C_FIRST, C_SECOND, C_THIRD, G_FIRST, G_SECOND, G_THIRD = 6, 9, 12, 13, 14, 17
STAGES = 20

STEPS = ("product", "z_first", "z_second", "hidden", "z_last", "pair_out", "down", "c_second", "c_third", "g_first", "g_second", "g_third", "store")
STARTS = (0.0, 1.5, 9.0, 14.0, 18.0, 22.0, 24.0, 30.0, 33.0, 35.5, 38.0, 41.0, 46.0)
SPACING = {"product": 3.0}
PAIR_SPACING = 11.0


def step_order():
    steps = []
    for at, step in enumerate(STEPS):
        for chunk in range(CHUNKS):
            spacing = SPACING.get(step, PAIR_SPACING)
            when = STARTS[at] + (chunk // 2) * spacing + (chunk % 2) * (1.5 if step == "product" else 0.1)
            steps.append((when, at, chunk, step))
    return [(step, chunk) for _, _, chunk, step in sorted(steps)]


def planes(first, second, codes):
    none = jnp.zeros_like(first)
    yield jnp.where(codes < 3, first, none)
    yield jnp.where(codes == 0, second, jnp.where((codes == 3) | (codes == 4), first, none))
    yield jnp.where((codes == 1) | (codes == 3), second, jnp.where(codes == 5, first, none))
    yield jnp.where((codes == 2) | (codes > 3), second, none)


def one_hot(shape, of_row):
    rows = lax.broadcasted_iota(jnp.int32, shape, 0)
    columns = lax.broadcasted_iota(jnp.int32, shape, 1)
    return jnp.where(columns == of_row(rows), 1.0, 0.0).astype(BF16)


def kernel(
    tok_h, gain_h, gv_h, gm_h, uv_h, um_h, dv_h, dm_h, out_h,
    tok, gain, gv, gm, uv, um, dv, dm, wgu, wd, wp, xp,
    part, pair_in, s1, z1_in, s2, z2_in, hid, dpart, c1_in, s3, c2_in, s4, c3_in, out,
    ssq, ssq_in, scale,
    load_sem, store_sem, send, recv, ssq_send, ssq_recv,
):
    row = lax.axis_index("row")
    col = lax.axis_index("col")
    k, c = row // 2, row % 2
    y, l, x = col // 8, (col // 4) % 2, col % 4
    width = gv.shape[1]
    features = tok.shape[1]

    def on_row(k2, c2):
        return (k2 * 2 + c2, col)

    def on_col(y2, l2, x2):
        return (row, (y2 * 2 + l2) * 4 + x2)

    partner = on_row(k, 1 - c)
    beside = on_row(k + 1 - 2 * (k % 2), c)
    across = on_row(3 - k, c)

    def z_of(chunk):
        if chunk % 2 == 0:
            return beside, across, ((k + 1) // 2) % 2, k // 2
        return across, beside, k // 2, k % 2

    def first_of(chunk):
        return x if chunk % 2 == 0 else y

    def second_of(chunk):
        return y if chunk % 2 == 0 else x

    def first_peer(chunk, d):
        if chunk % 2 == 0:
            return on_col(y, l, (x + d) % 4)
        return on_col((y + d) % 4, l, x)

    def second_peer(chunk, d):
        return first_peer(chunk + 1, d)

    sources = (gv_h, gm_h, tok_h, gain_h, uv_h, um_h, dv_h, dm_h)
    places = (gv, gm, tok, gain, uv, um, dv, dm)
    loads = [pltpu.make_async_copy(a, b, load_sem.at[n]) for n, (a, b) in enumerate(zip(sources, places))]
    for load in loads:
        load.start()

    barrier = pltpu.get_barrier_semaphore()
    peers = [((row + d) % 8, col) for d in range(1, 8)]
    for d in range(1, 4):
        peers += [on_col(y, l, (x + d) % 4), on_col((y + d) % 4, l, x)]
    peers.append(on_col(y, 1 - l, x))
    for peer in peers:
        pl.semaphore_signal(barrier, inc=1, device_id=peer, device_id_type=MESH)

    split_gu = one_hot((128, 128), lambda r: jnp.where(r < 64, 2 * r, 2 * r - 127))
    split_d = one_hot((64, 64), lambda r: jnp.where(r < 32, 2 * r, 2 * r - 63))
    mix_d = one_hot((128, 128), lambda r: (r & 3) * 32 + (r >> 2))
    mix_x = one_hot((256, 256), lambda r: (r & 3) * 64 + (r >> 2))

    def expand_gu(vals, meta, offset):
        def block(b, carry):
            for j in range(width // 128):
                at = slice(j * 128, (j + 1) * 128)
                v = vals[pl.ds(pl.multiple_of(b * 128, 128), 128), at]
                both = jnp.dot(split_gu, v, preferred_element_type=F32)
                codes = meta[pl.ds(pl.multiple_of(b * 64, 64), 64), at]
                for p, plane in enumerate(planes(both[:64], both[64:], codes)):
                    wgu[pl.ds(pl.multiple_of(b * 256 + p * 64, 64), 64), offset + j * 128 : offset + (j + 1) * 128] = plane.astype(BF16)
            return carry

        lax.fori_loop(0, vals.shape[0] // 128, block, 0)

    def expand_d(b, carry):
        for j in range(wd.shape[1] // 256):
            at = slice(j * 256, (j + 1) * 256)
            v = dv[pl.ds(pl.multiple_of(b * 64, 64), 64), at]
            both = jnp.dot(split_d, v, preferred_element_type=F32)
            codes = dm[pl.ds(pl.multiple_of(b * 32, 32), 32), at]
            for p, plane in enumerate(planes(both[:32], both[32:], codes)):
                wp[p * 32 : (p + 1) * 32, :] = plane.astype(BF16)
            dense = jnp.dot(mix_d, wp[...], preferred_element_type=F32)
            wd[pl.ds(pl.multiple_of(b * 128, 128), 128), at] = dense.astype(BF16)
        return carry

    loads[0].wait()
    loads[1].wait()
    expand_gu(gv, gm, 0)
    loads[4].wait()
    loads[5].wait()
    expand_gu(uv, um, width)
    loads[2].wait()
    loads[3].wait()
    pl.semaphore_wait(barrier, len(peers))

    def copy(src, dst, chunk, stage, to):
        return pltpu.make_async_remote_copy(
            src_ref=src, dst_ref=dst, send_sem=send.at[chunk, stage], recv_sem=recv.at[chunk, stage],
            device_id=to, device_id_type=MESH,
        )

    def arrive(dst, chunk, stage):
        copy(dst, dst, chunk, stage, partner).wait_recv()

    def ssq_copy(d):
        return pltpu.make_async_remote_copy(
            src_ref=ssq, dst_ref=ssq_in.at[d - 1], send_sem=ssq_send.at[d - 1], recv_sem=ssq_recv.at[d - 1],
            device_id=((row + d) % 8, col), device_id_type=MESH,
        )

    def product(i):
        xf = tok[i * ROWS : (i + 1) * ROWS, :].astype(F32)
        sums = jnp.sum(xf * xf, axis=1, keepdims=True)
        square = (ROWS, ROWS)
        diagonal = lax.broadcasted_iota(jnp.int32, square, 0) == lax.broadcasted_iota(jnp.int32, square, 1)
        ssq[i : i + 1, :] = jnp.sum(jnp.where(diagonal, sums, 0.0), axis=0, keepdims=True)
        weighted = (xf * gain[...]).astype(BF16)
        for b in range(features // 256):
            at = slice(b * 256, (b + 1) * 256)
            xp[:, at] = jnp.dot(weighted[:, at], mix_x, preferred_element_type=F32).astype(BF16)

        def tile(n, carry):
            at = pl.ds(pl.multiple_of(n * 256, 256), 256)
            sums = jnp.dot(xp[...], wgu[:, at], preferred_element_type=F32).astype(BF16)
            part[i, :, :, :, :, at] = sums.reshape(2, 2, 2, PIECE, 256)
            return carry

        lax.fori_loop(0, wgu.shape[1] // 256, tile, 0)
        copy(part.at[i, 1 - c], pair_in.at[i], i, PAIR_IN, partner).start()
        if i == CHUNKS - 1:
            for d in range(1, 8):
                ssq_copy(d).start()

    def z_first(i):
        p1, _, h, u = z_of(i)
        arrive(pair_in.at[i], i, PAIR_IN)
        s1[i] = (part[i, c, 1 - h].astype(F32) + pair_in[i, 1 - h].astype(F32)).astype(BF16)
        copy(s1.at[i], z1_in.at[i], i, Z_FIRST, p1).start()

    def held(i, h, u):
        return part[i, c, h, u].astype(F32) + pair_in[i, h, u].astype(F32) + z1_in[i, u].astype(F32)

    def z_second(i):
        _, p2, h, u = z_of(i)
        arrive(z1_in.at[i], i, Z_FIRST)
        s2[i] = held(i, h, 1 - u).astype(BF16)
        copy(s2.at[i], z2_in.at[i], i, Z_SECOND, p2).start()

    def hidden(i):
        _, p2, h, u = z_of(i)
        if i == 0:
            total = ssq[...]
            for d in range(1, 8):
                ssq_copy(d).wait_recv()
                total = total + ssq_in[d - 1]
            scale[...] = lax.rsqrt(total / (features * 8) + EPS)
        lanes = (PIECE, ROWS)
        mine = c * 64 + (2 * h + u) * PIECE + lax.broadcasted_iota(jnp.int32, lanes, 0)
        chosen = lax.broadcasted_iota(jnp.int32, lanes, 1) == mine
        factor = jnp.sum(jnp.where(chosen, scale[i : i + 1, :], 0.0), axis=1, keepdims=True)
        arrive(z2_in.at[i], i, Z_SECOND)
        sums = (held(i, h, u) + z2_in[i].astype(F32)) * factor
        gate, up = sums[:, :width], sums[:, width:]
        hid[i, c, h, u] = (gate / (1.0 + jnp.exp(-gate)) * up).astype(BF16)
        copy(hid.at[i, c, h, u], hid.at[i, c, h, u], i, Z_BACK, p2).start()

    def z_last(i):
        p1, _, h, u = z_of(i)
        arrive(hid.at[i, c, h, 1 - u], i, Z_BACK)
        copy(hid.at[i, c, h], hid.at[i, c, h], i, Z_LAST, p1).start()

    def pair_out(i):
        _, _, h, _ = z_of(i)
        arrive(hid.at[i, c, 1 - h], i, Z_LAST)
        copy(hid.at[i, c], hid.at[i, c], i, PAIR_OUT, partner).start()

    def down(i):
        if i == 0:
            loads[6].wait()
            loads[7].wait()
            lax.fori_loop(0, dv.shape[0] // 64, expand_d, 0)
        arrive(hid.at[i, 1 - c], i, PAIR_OUT)

        def tile(n, carry):
            at = pl.ds(pl.multiple_of(n * 256, 256), 256)
            sums = jnp.dot(hid[i].reshape(ROWS, width), wd[:, at], preferred_element_type=F32).astype(BF16)
            dpart[i, :, :, at] = sums.reshape(4, 32, 256)
            return carry

        lax.fori_loop(0, wd.shape[1] // 256, tile, 0)
        a = first_of(i)
        for d in range(1, 4):
            copy(dpart.at[i, (a + d) % 4], c1_in.at[i, d - 1], i, C_FIRST + d - 1, first_peer(i, d)).start()

    def c_second(i):
        a, b = first_of(i), second_of(i)
        total = dpart[i, a].astype(F32)
        for d in range(1, 4):
            arrive(c1_in.at[i, d - 1], i, C_FIRST + d - 1)
            total = total + c1_in[i, d - 1].astype(F32)
        total = total.astype(BF16)
        for q in range(4):
            s3[i, q] = total[:, q * 256 : (q + 1) * 256]
        for d in range(1, 4):
            copy(s3.at[i, (b + d) % 4], c2_in.at[i, d - 1], i, C_SECOND + d - 1, second_peer(i, d)).start()

    def c_third(i):
        total = s3[i, second_of(i)].astype(F32)
        for d in range(1, 4):
            arrive(c2_in.at[i, d - 1], i, C_SECOND + d - 1)
            total = total + c2_in[i, d - 1].astype(F32)
        total = total.astype(BF16)
        for q in range(2):
            s4[i, q] = total[:, q * 128 : (q + 1) * 128]
        copy(s4.at[i, 1 - l], c3_in.at[i], i, C_THIRD, on_col(y, 1 - l, x)).start()

    def columns_of(i, place):
        return pl.ds(pl.multiple_of(second_of(i) * 256 + place * 128, 128), 128)

    def g_first(i):
        a = first_of(i)
        at = columns_of(i, l)
        arrive(c3_in.at[i], i, C_THIRD)
        own = tok[pl.ds(pl.multiple_of(i * ROWS + a * 32, 32), 32), at].astype(F32)
        out[i, a, :, at] = (own + s4[i, l].astype(F32) + c3_in[i].astype(F32)).astype(BF16)
        copy(out.at[i, a, :, at], out.at[i, a, :, at], i, G_FIRST, on_col(y, 1 - l, x)).start()

    def block_of(i, b):
        return out.at[i, first_of(i), :, pl.ds(pl.multiple_of(b * 256, 256), 256)]

    def g_second(i):
        arrive(out.at[i, first_of(i), :, columns_of(i, 1 - l)], i, G_FIRST)
        mine = block_of(i, second_of(i))
        for d in range(1, 4):
            copy(mine, mine, i, G_SECOND + d - 1, second_peer(i, d)).start()

    def g_third(i):
        a, b = first_of(i), second_of(i)
        for d in range(1, 4):
            arrive(block_of(i, (b + 4 - d) % 4), i, G_SECOND + d - 1)
        for d in range(1, 4):
            copy(out.at[i, a], out.at[i, a], i, G_THIRD + d - 1, first_peer(i, d)).start()

    def stored(i):
        return pltpu.make_async_copy(out.at[i], out_h.at[i], store_sem.at[i])

    def store(i):
        a = first_of(i)
        for d in range(1, 4):
            arrive(out.at[i, (a + 4 - d) % 4], i, G_THIRD + d - 1)
        stored(i).start()

    bodies = dict(
        product=product, z_first=z_first, z_second=z_second, hidden=hidden, z_last=z_last, pair_out=pair_out, down=down,
        c_second=c_second, c_third=c_third, g_first=g_first, g_second=g_second, g_third=g_third, store=store,
    )
    for step, chunk in step_order():
        bodies[step](chunk)

    def sent(src, chunk, stage):
        copy(src, src, chunk, stage, partner).wait_send()

    def finish(i, carry):
        sent(pair_in.at[i], i, PAIR_IN)
        sent(s1.at[i], i, Z_FIRST)
        sent(s2.at[i], i, Z_SECOND)
        sent(hid.at[i, 0, 0, 0], i, Z_BACK)
        sent(hid.at[i, 0, 0], i, Z_LAST)
        sent(hid.at[i, 0], i, PAIR_OUT)
        sent(c3_in.at[i], i, C_THIRD)
        sent(c3_in.at[i], i, G_FIRST)
        for d in range(3):
            sent(c1_in.at[i, d], i, C_FIRST + d)
            sent(c2_in.at[i, d], i, C_SECOND + d)
            sent(c2_in.at[i, d], i, G_SECOND + d)
            sent(c1_in.at[i, d], i, G_THIRD + d)
        stored(i).wait()
        return carry

    lax.fori_loop(0, CHUNKS, finish, 0)
    for d in range(1, 8):
        ssq_copy(d).wait_send()


def per_device(tokens, norm_gain, gate_vals, gate_meta, up_vals, up_meta, down_vals, down_meta):
    batch, features = tokens.shape
    width = gate_vals.shape[1]
    pieces = (2, 2, PIECE)
    vmem = pltpu.VMEM
    scratch = [
        vmem(tokens.shape, BF16), vmem((1, features), F32),
        vmem(gate_vals.shape, BF16), vmem(gate_meta.shape, jnp.int32),
        vmem(up_vals.shape, BF16), vmem(up_meta.shape, jnp.int32),
        vmem(down_vals.shape, BF16), vmem(down_meta.shape, jnp.int32),
        vmem((features, 2 * width), BF16), vmem((width, features), BF16), vmem((128, 256), BF16), vmem((ROWS, features), BF16),
        vmem((CHUNKS, 2, *pieces, 2 * width), BF16), vmem((CHUNKS, *pieces, 2 * width), BF16),
        vmem((CHUNKS, 2, PIECE, 2 * width), BF16), vmem((CHUNKS, 2, PIECE, 2 * width), BF16),
        vmem((CHUNKS, PIECE, 2 * width), BF16), vmem((CHUNKS, PIECE, 2 * width), BF16),
        vmem((CHUNKS, 2, *pieces, width), BF16),
        vmem((CHUNKS, 4, 32, features), BF16), vmem((CHUNKS, 3, 32, features), BF16),
        vmem((CHUNKS, 4, 32, 256), BF16), vmem((CHUNKS, 3, 32, 256), BF16),
        vmem((CHUNKS, 2, 32, 128), BF16), vmem((CHUNKS, 32, 128), BF16),
        vmem((CHUNKS, 4, 32, features), BF16),
        vmem((CHUNKS, ROWS), F32), vmem((7, CHUNKS, ROWS), F32), vmem((CHUNKS, ROWS), F32),
        pltpu.SemaphoreType.DMA((8,)), pltpu.SemaphoreType.DMA((CHUNKS,)),
        pltpu.SemaphoreType.DMA((CHUNKS, STAGES)), pltpu.SemaphoreType.DMA((CHUNKS, STAGES)),
        pltpu.SemaphoreType.DMA((7,)), pltpu.SemaphoreType.DMA((7,)),
    ]
    anywhere = pl.BlockSpec(memory_space=pl.ANY)
    out = pl.pallas_call(
        kernel,
        out_shape=jax.ShapeDtypeStruct((CHUNKS, 4, 32, features), BF16),
        in_specs=[anywhere] * 8,
        out_specs=anywhere,
        scratch_shapes=scratch,
        compiler_params=pltpu.CompilerParams(collective_id=0, has_side_effects=True, vmem_limit_bytes=60 * 1024 * 1024),
    )(tokens, norm_gain.reshape(1, features), gate_vals, gate_meta, up_vals, up_meta, down_vals, down_meta)
    return out.reshape(batch, features)


def solution(mesh):
    return jax.shard_map(
        per_device,
        mesh=mesh,
        in_specs=(
            P(None, "row"),
            P("row"),
            P("row", "col"),
            P("row", "col"),
            P("row", "col"),
            P("row", "col"),
            P("col", "row"),
            P("col", "row"),
        ),
        out_specs=P(None, "row"),
        check_vma=False,
    )
```

```python
import functools

import jax
import jax.numpy as jnp
from jax import lax
from jax.experimental import pallas as pl
from jax.experimental.pallas import tpu as pltpu
from jax.sharding import PartitionSpec as P

EPS = 1e-05
MESH = pl.DeviceIdType.MESH
F32 = jnp.float32
BF16 = jnp.bfloat16

CHUNKS = 8
ROWS = 128
PIECE = 16

PAIR_IN, Z_FIRST, Z_SECOND, Z_BACK, Z_LAST, PAIR_OUT, BETWEEN = range(7)
F_OUT, S_OUT, S_BACK, F_BACK = 7, 10, 13, 16
STAGES = 19

STEPS = (
    "squares", "expand_down", "product", "z_first", "z_second", "hidden", "z_last", "pair_out", "down", "s_out", "between", "s_back",
    "f_back", "store",
)
ORDER = (
    16, 0, 24, 25, 22, 18, 20, 26, 31, 32, 27, 29, 28, 33, 30, 40, 34, 8, 36, 41, 35, 39, 37, 49,
    42, 43, 38, 48, 44, 45, 57, 50, 51, 56, 65, 47, 46, 64, 52, 53, 58, 59, 66, 55, 67, 54, 60, 73,
    61, 72, 68, 69, 62, 63, 75, 74, 80, 70, 81, 76, 71, 77, 88, 89, 83, 82, 84, 85, 91, 78, 90, 79,
    92, 97, 96, 86, 99, 93, 87, 100, 104, 94, 95, 105, 98, 101, 107, 102, 108, 103, 109, 106, 111, 110,
)


def step_order():
    return [(STEPS[n // CHUNKS], n % CHUNKS) for n in ORDER]


def planes(first, second, codes):
    none = jnp.zeros_like(first)
    yield jnp.where(codes < 3, first, none)
    yield jnp.where(codes == 0, second, jnp.where((codes == 3) | (codes == 4), first, none))
    yield jnp.where((codes == 1) | (codes == 3), second, jnp.where(codes == 5, first, none))
    yield jnp.where((codes == 2) | (codes > 3), second, none)


def one_hot(shape, of_row):
    rows = lax.broadcasted_iota(jnp.int32, shape, 0)
    columns = lax.broadcasted_iota(jnp.int32, shape, 1)
    return jnp.where(columns == of_row(rows), 1.0, 0.0).astype(BF16)


def kernel(
    tok_h, gain_h, gv_h, gm_h, uv_h, um_h, dv_h, dm_h, out_h,
    tok, gain, gv, gm, uv, um, dv, dm, wgu, wd, wp, xp,
    part, pair_in, s1, z1_in, s2, z2_in, hid, dpart, f_in, s4, s_in, s5, t_in, out,
    ssq, ssq_in, scale,
    load_sem, store_sem, send, recv, ssq_send, ssq_recv,
):
    row = lax.axis_index("row")
    col = lax.axis_index("col")
    k, c = row // 2, row % 2
    y, l, x = col // 8, (col // 4) % 2, col % 4
    width = gv.shape[1]
    features = tok.shape[1]

    def on_row(k2, c2):
        return (k2 * 2 + c2, col)

    def on_col(y2, l2, x2):
        return (row, (y2 * 2 + l2) * 4 + x2)

    partner = on_row(k, 1 - c)

    def ways(n, way):
        if way == 0:
            return n + 1 - 2 * (n % 2), 3 - n, ((n + 1) // 2) % 2, n // 2
        return 3 - n, n + 1 - 2 * (n % 2), n // 2, n % 2

    def z_of(chunk):
        p1, p2, h, u = ways(k, chunk % 2)
        return on_row(p1, c), on_row(p2, c), h, u

    def first_of(chunk):
        return x if chunk % 2 == 0 else y

    def second_of(chunk):
        return y if chunk % 2 == 0 else x

    def first_peer(chunk, d):
        if chunk % 2 == 0:
            return on_col(y, l, (x + d) % 4)
        return on_col((y + d) % 4, l, x)

    def second_peer(chunk, d):
        return first_peer(chunk + 1, d)

    opposite = on_col(y, 1 - l, x)

    sources = (gv_h, gm_h, tok_h, gain_h, uv_h, um_h, dv_h, dm_h)
    places = (gv, gm, tok, gain, uv, um, dv, dm)
    loads = [pltpu.make_async_copy(a, b, load_sem.at[n]) for n, (a, b) in enumerate(zip(sources, places))]
    for load in loads:
        load.start()

    barrier = pltpu.get_barrier_semaphore()
    peers = [((row + d) % 8, col) for d in range(1, 8)]
    for d in range(1, 4):
        peers += [on_col(y, l, (x + d) % 4), on_col((y + d) % 4, l, x)]
    peers.append(on_col(y, 1 - l, x))
    for peer in peers:
        pl.semaphore_signal(barrier, inc=1, device_id=peer, device_id_type=MESH)

    split_gu = one_hot((128, 128), lambda r: jnp.where(r < 64, 2 * r, 2 * r - 127))
    split_d = one_hot((64, 64), lambda r: jnp.where(r < 32, 2 * r, 2 * r - 63))
    mix_d = one_hot((128, 128), lambda r: (r & 3) * 32 + (r >> 2))
    mix_x = one_hot((256, 256), lambda r: (r & 3) * 64 + (r >> 2))

    def expand_gu(vals, meta, offset):
        def block(b, carry):
            for j in range(width // 128):
                at = slice(j * 128, (j + 1) * 128)
                v = vals[pl.ds(pl.multiple_of(b * 128, 128), 128), at]
                both = jnp.dot(split_gu, v, preferred_element_type=F32)
                codes = meta[pl.ds(pl.multiple_of(b * 64, 64), 64), at]
                for p, plane in enumerate(planes(both[:64], both[64:], codes)):
                    wgu[pl.ds(pl.multiple_of(b * 256 + p * 64, 64), 64), offset + j * 128 : offset + (j + 1) * 128] = plane.astype(BF16)
            return carry

        lax.fori_loop(0, vals.shape[0] // 128, block, 0)

    def expand_d(b, carry):
        for j in range(wd.shape[1] // 256):
            at = slice(j * 256, (j + 1) * 256)
            v = dv[pl.ds(pl.multiple_of(b * 64, 64), 64), at]
            both = jnp.dot(split_d, v, preferred_element_type=F32)
            codes = dm[pl.ds(pl.multiple_of(b * 32, 32), 32), at]
            for p, plane in enumerate(planes(both[:32], both[32:], codes)):
                wp[p * 32 : (p + 1) * 32, :] = plane.astype(BF16)
            dense = jnp.dot(mix_d, wp[...], preferred_element_type=F32)
            wd[pl.ds(pl.multiple_of(b * 128, 128), 128), at] = dense.astype(BF16)
        return carry

    loads[0].wait()
    loads[1].wait()
    expand_gu(gv, gm, 0)
    loads[4].wait()
    loads[5].wait()
    expand_gu(uv, um, width)
    loads[2].wait()
    loads[3].wait()

    def copy(src, dst, chunk, stage, to):
        return pltpu.make_async_remote_copy(
            src_ref=src, dst_ref=dst, send_sem=send.at[chunk, stage], recv_sem=recv.at[chunk, stage],
            device_id=to, device_id_type=MESH,
        )

    def arrive(dst, chunk, stage):
        copy(dst, dst, chunk, stage, partner).wait_recv()

    def ssq_copy(d):
        return pltpu.make_async_remote_copy(
            src_ref=ssq, dst_ref=ssq_in.at[d - 1], send_sem=ssq_send.at[d - 1], recv_sem=ssq_recv.at[d - 1],
            device_id=((row + d) % 8, col), device_id_type=MESH,
        )

    def squares(i):
        def rows(n, carry):
            xf = tok[pl.ds(pl.multiple_of(n * ROWS, ROWS), ROWS), :].astype(F32)
            sums = jnp.sum(xf * xf, axis=1, keepdims=True)
            square = (ROWS, ROWS)
            diagonal = lax.broadcasted_iota(jnp.int32, square, 0) == lax.broadcasted_iota(jnp.int32, square, 1)
            ssq[pl.ds(n, 1), :] = jnp.sum(jnp.where(diagonal, sums, 0.0), axis=0, keepdims=True)
            return carry

        lax.fori_loop(0, CHUNKS, rows, 0)
        for d in range(1, 8):
            ssq_copy(d).start()

    first_chunk = min(ORDER, key=lambda n: n // CHUNKS != 2) % CHUNKS

    def product(i):
        weighted = (tok[i * ROWS : (i + 2) * ROWS, :].astype(F32) * gain[...]).astype(BF16)
        for b in range(features // 256):
            at = slice(b * 256, (b + 1) * 256)
            xp[:, at] = jnp.dot(weighted[:, at], mix_x, preferred_element_type=F32).astype(BF16)
        for n in range(2 * width // 256):
            at = slice(n * 256, (n + 1) * 256)
            sums = jnp.dot(xp[...], wgu[:, at], preferred_element_type=F32).astype(BF16)
            part[i : i + 2, :, :, :, :, at] = sums.reshape(2, 2, 2, 2, PIECE, 256)
        if i == first_chunk:
            pl.semaphore_wait(barrier, len(peers))
        for j in (i, i + 1):
            copy(part.at[j, 1 - c], pair_in.at[j], j, PAIR_IN, partner).start()

    def z_first(i):
        p1, _, h, u = z_of(i)
        arrive(pair_in.at[i], i, PAIR_IN)
        s1[i] = (part[i, c, 1 - h].astype(F32) + pair_in[i, 1 - h].astype(F32)).astype(BF16)
        copy(s1.at[i], z1_in.at[i], i, Z_FIRST, p1).start()

    def held(i, h, u):
        return part[i, c, h, u].astype(F32) + pair_in[i, h, u].astype(F32) + z1_in[i, u].astype(F32)

    def z_second(i):
        _, p2, h, u = z_of(i)
        arrive(z1_in.at[i], i, Z_FIRST)
        s2[i] = held(i, h, 1 - u).astype(BF16)
        copy(s2.at[i], z2_in.at[i], i, Z_SECOND, p2).start()

    def hidden(i):
        _, p2, h, u = z_of(i)
        if i == 0:
            total = ssq[...]
            for d in range(1, 8):
                ssq_copy(d).wait_recv()
                total = total + ssq_in[d - 1]
            scale[...] = lax.rsqrt(total / (features * 8) + EPS)
        lanes = (PIECE, ROWS)
        mine = c * 64 + (2 * h + u) * PIECE + lax.broadcasted_iota(jnp.int32, lanes, 0)
        chosen = lax.broadcasted_iota(jnp.int32, lanes, 1) == mine
        factor = jnp.sum(jnp.where(chosen, scale[i : i + 1, :], 0.0), axis=1, keepdims=True)
        arrive(z2_in.at[i], i, Z_SECOND)
        sums = (held(i, h, u) + z2_in[i].astype(F32)) * factor
        gate, up = sums[:, :width], sums[:, width:]
        hid[i, c, h, u] = (gate / (1.0 + jnp.exp(-gate)) * up).astype(BF16)
        copy(hid.at[i, c, h, u], hid.at[i, c, h, u], i, Z_BACK, p2).start()

    def z_last(i):
        p1, _, h, u = z_of(i)
        arrive(hid.at[i, c, h, 1 - u], i, Z_BACK)
        copy(hid.at[i, c, h], hid.at[i, c, h], i, Z_LAST, p1).start()

    def pair_out(i):
        _, _, h, _ = z_of(i)
        arrive(hid.at[i, c, 1 - h], i, Z_LAST)
        copy(hid.at[i, c], hid.at[i, c], i, PAIR_OUT, partner).start()

    def expand_down(i):
        loads[6].wait()
        loads[7].wait()
        lax.fori_loop(0, dv.shape[0] // 64, expand_d, 0)

    def down(i):
        arrive(hid.at[i, 1 - c], i, PAIR_OUT)
        for n in range(wd.shape[1] // 256):
            at = slice(n * 256, (n + 1) * 256)
            sums = jnp.dot(hid[i].reshape(ROWS, width), wd[:, at], preferred_element_type=F32).astype(BF16)
            dpart[i, :, :, at] = sums.reshape(4, 32, 256)
        a = first_of(i)
        for d in range(1, 4):
            copy(dpart.at[i, (a + d) % 4], f_in.at[i, d - 1], i, F_OUT + d - 1, first_peer(i, d)).start()

    def s_out(i):
        a, b = first_of(i), second_of(i)
        total = dpart[i, a].astype(F32)
        for d in range(1, 4):
            arrive(f_in.at[i, d - 1], i, F_OUT + d - 1)
            total = total + f_in[i, d - 1].astype(F32)
        total = total.astype(BF16)
        for q in range(4):
            s4[i, q] = total[:, q * 256 : (q + 1) * 256]
        for d in range(1, 4):
            copy(s4.at[i, (b + d) % 4], s_in.at[i, d - 1], i, S_OUT + d - 1, second_peer(i, d)).start()

    def between(i):
        total = s4[i, second_of(i)].astype(F32)
        for d in range(1, 4):
            arrive(s_in.at[i, d - 1], i, S_OUT + d - 1)
            total = total + s_in[i, d - 1].astype(F32)
        s5[i] = total.astype(BF16)
        copy(s5.at[i], t_in.at[i], i, BETWEEN, opposite).start()

    def columns_of(b):
        return pl.ds(pl.multiple_of(b * 256, 256), 256)

    def s_back(i):
        a, b = first_of(i), second_of(i)
        own = tok[pl.ds(pl.multiple_of(i * ROWS + a * 32, 32), 32), columns_of(b)].astype(F32)
        arrive(t_in.at[i], i, BETWEEN)
        out[i, a, :, columns_of(b)] = (own + (s5[i].astype(F32) + t_in[i].astype(F32))).astype(BF16)
        mine = out.at[i, a, :, columns_of(b)]
        for d in range(1, 4):
            copy(mine, mine, i, S_BACK + d - 1, second_peer(i, d)).start()

    def f_back(i):
        a, b = first_of(i), second_of(i)
        for d in range(1, 4):
            arrive(out.at[i, a, :, columns_of((b + 4 - d) % 4)], i, S_BACK + d - 1)
        for d in range(1, 4):
            copy(out.at[i, a], out.at[i, a], i, F_BACK + d - 1, first_peer(i, d)).start()

    def stored(i):
        return pltpu.make_async_copy(out.at[i], out_h.at[i], store_sem.at[i])

    def store(i):
        a = first_of(i)
        for d in range(1, 4):
            arrive(out.at[i, (a + 4 - d) % 4], i, F_BACK + d - 1)
        stored(i).start()

    bodies = dict(
        squares=squares, product=product, z_first=z_first, z_second=z_second, hidden=hidden, z_last=z_last, pair_out=pair_out,
        expand_down=expand_down, down=down, s_out=s_out, between=between, s_back=s_back, f_back=f_back, store=store,
    )
    order = step_order()
    for step, chunk in order:
        bodies[step](chunk)

    def sent(src, chunk, stage):
        copy(src, src, chunk, stage, partner).wait_send()

    def finish(i, carry):
        sent(pair_in.at[i], i, PAIR_IN)
        sent(s1.at[i], i, Z_FIRST)
        sent(s2.at[i], i, Z_SECOND)
        sent(hid.at[i, 0, 0, 0], i, Z_BACK)
        sent(hid.at[i, 0, 0], i, Z_LAST)
        sent(hid.at[i, 0], i, PAIR_OUT)
        sent(t_in.at[i], i, BETWEEN)
        for d in range(3):
            sent(f_in.at[i, d], i, F_OUT + d)
            sent(s_in.at[i, d], i, S_OUT + d)
            sent(s_in.at[i, d], i, S_BACK + d)
            sent(f_in.at[i, d], i, F_BACK + d)
        stored(i).wait()
        return carry

    lax.fori_loop(0, CHUNKS, finish, 0)
    for d in range(1, 8):
        ssq_copy(d).wait_send()


def per_device(tokens, norm_gain, gate_vals, gate_meta, up_vals, up_meta, down_vals, down_meta):
    batch, features = tokens.shape
    width = gate_vals.shape[1]
    pieces = (2, 2, PIECE)
    vmem = pltpu.VMEM
    scratch = [
        vmem(tokens.shape, BF16), vmem((1, features), F32),
        vmem(gate_vals.shape, BF16), vmem(gate_meta.shape, jnp.int32),
        vmem(up_vals.shape, BF16), vmem(up_meta.shape, jnp.int32),
        vmem(down_vals.shape, BF16), vmem(down_meta.shape, jnp.int32),
        vmem((features, 2 * width), BF16), vmem((width, features), BF16), vmem((128, 256), BF16), vmem((2 * ROWS, features), BF16),
        vmem((CHUNKS, 2, *pieces, 2 * width), BF16), vmem((CHUNKS, *pieces, 2 * width), BF16),
        vmem((CHUNKS, 2, PIECE, 2 * width), BF16), vmem((CHUNKS, 2, PIECE, 2 * width), BF16),
        vmem((CHUNKS, PIECE, 2 * width), BF16), vmem((CHUNKS, PIECE, 2 * width), BF16),
        vmem((CHUNKS, 2, *pieces, width), BF16),
        vmem((CHUNKS, 4, 32, features), BF16), vmem((CHUNKS, 3, 32, features), BF16),
        vmem((CHUNKS, 4, 32, 256), BF16), vmem((CHUNKS, 3, 32, 256), BF16),
        vmem((CHUNKS, 32, 256), BF16), vmem((CHUNKS, 32, 256), BF16),
        vmem((CHUNKS, 4, 32, features), BF16),
        vmem((CHUNKS, ROWS), F32), vmem((7, CHUNKS, ROWS), F32), vmem((CHUNKS, ROWS), F32),
        pltpu.SemaphoreType.DMA((8,)), pltpu.SemaphoreType.DMA((CHUNKS,)),
        pltpu.SemaphoreType.DMA((CHUNKS, STAGES)), pltpu.SemaphoreType.DMA((CHUNKS, STAGES)),
        pltpu.SemaphoreType.DMA((7,)), pltpu.SemaphoreType.DMA((7,)),
    ]
    anywhere = pl.BlockSpec(memory_space=pl.ANY)
    out = pl.pallas_call(
        kernel,
        out_shape=jax.ShapeDtypeStruct((CHUNKS, 4, 32, features), BF16),
        in_specs=[anywhere] * 8,
        out_specs=anywhere,
        scratch_shapes=scratch,
        compiler_params=pltpu.CompilerParams(collective_id=0, has_side_effects=True, vmem_limit_bytes=60 * 1024 * 1024),
    )(tokens, norm_gain.reshape(1, features), gate_vals, gate_meta, up_vals, up_meta, down_vals, down_meta)
    return out.reshape(batch, features)


def solution(mesh):
    return jax.shard_map(
        per_device,
        mesh=mesh,
        in_specs=(
            P(None, "row"),
            P("row"),
            P("row", "col"),
            P("row", "col"),
            P("row", "col"),
            P("row", "col"),
            P("col", "row"),
            P("col", "row"),
        ),
        out_specs=P(None, "row"),
        check_vma=False,
    )
```

```python
import functools

import jax
import jax.numpy as jnp
from jax import lax
from jax.experimental import pallas as pl
from jax.experimental.pallas import tpu as pltpu
from jax.sharding import PartitionSpec as P

EPS = 1e-05
MESH = pl.DeviceIdType.MESH
F32 = jnp.float32
BF16 = jnp.bfloat16

CHUNKS = 8
ROWS = 128
PIECE = 16

PAIR_IN, Z_FIRST, Z_SECOND, Z_BACK, Z_LAST, PAIR_OUT, F_OUT, S_OUT, BETWEEN, S_BACK, F_BACK = range(11)
STAGES = 11

STEPS = (
    "squares", "expand_down", "product", "z_first", "z_second", "hidden", "z_last", "pair_out", "down", "s_out", "between", "s_back",
    "f_back", "arrive",
)
ORDER = (
    18, 0, 26, 27, 16, 25, 20, 34, 24, 29, 22, 42, 33, 30, 8, 32, 50, 41, 28, 35, 38, 58, 31, 49,
    40, 37, 43, 46, 36, 66, 39, 48, 57, 45, 74, 65, 54, 51, 44, 47, 56, 53, 64, 62, 59, 82, 73, 70,
    52, 67, 55, 61, 72, 81, 69, 78, 90, 60, 75, 89, 63, 68, 80, 77, 71, 86, 83, 98, 76, 85, 94, 88,
    91, 79, 97, 84, 93, 106, 102, 99, 87, 92, 105, 96, 95, 101, 110, 100, 107, 104, 103, 109, 108, 111,
)


def step_order():
    return [(STEPS[n // CHUNKS], n % CHUNKS) for n in ORDER]


def planes(first, second, codes):
    none = jnp.zeros_like(first)
    yield jnp.where(codes < 3, first, none)
    yield jnp.where(codes == 0, second, jnp.where((codes == 3) | (codes == 4), first, none))
    yield jnp.where((codes == 1) | (codes == 3), second, jnp.where(codes == 5, first, none))
    yield jnp.where((codes == 2) | (codes > 3), second, none)


def one_hot(shape, of_row):
    rows = lax.broadcasted_iota(jnp.int32, shape, 0)
    columns = lax.broadcasted_iota(jnp.int32, shape, 1)
    return jnp.where(columns == of_row(rows), 1.0, 0.0).astype(BF16)


def kernel(
    tok_h, gain_h, gv_h, gm_h, uv_h, um_h, dv_h, dm_h, out,
    tok, gain, gv, gm, uv, um, dv, dm, wgu, wd, wp, xp,
    part, pair_in, s1, z1_in, s2, z2_in, hid, dpart, f_in, s4, s_in, s5, t_in,
    ssq, ssq_in, scale,
    load_sem, send, recv, ssq_sem,
):
    row = lax.axis_index("row")
    col = lax.axis_index("col")
    k, c = row // 2, row % 2
    y, l, x = col // 8, (col // 4) % 2, col % 4
    width = gv.shape[1]
    features = tok.shape[1]

    def on_row(k2, c2):
        return (k2 * 2 + c2, col)

    def on_col(y2, l2, x2):
        return (row, (y2 * 2 + l2) * 4 + x2)

    partner = on_row(k, 1 - c)

    def ways(n, way):
        near, far = n + 1 - 2 * (n % 2), 3 - n
        return (near, far) if way == 0 else (far, near)

    def z_of(way):
        p1, p2 = ways(k, way)
        return p1, p2, ways(p1, way)[1]

    def to_z(n):
        return on_row(n, c)

    def first_of(v):
        return x if v == 0 else y

    def second_of(v):
        return y if v == 0 else x

    def first_peer(v, d):
        if v == 0:
            return on_col(y, l, (x + d) % 4)
        return on_col((y + d) % 4, l, x)

    def second_peer(v, d):
        return first_peer(1 - v, d)

    opposite = on_col(y, 1 - l, x)

    sources = (gv_h, gm_h, tok_h, gain_h, uv_h, um_h, dv_h, dm_h)
    places = (gv, gm, tok, gain, uv, um, dv, dm)
    loads = [pltpu.make_async_copy(a, b, load_sem.at[n]) for n, (a, b) in enumerate(zip(sources, places))]
    for load in loads:
        load.start()

    barrier = pltpu.get_barrier_semaphore()
    peers = [((row + d) % 8, col) for d in range(1, 8)]
    for d in range(1, 4):
        peers += [on_col(y, l, (x + d) % 4), on_col((y + d) % 4, l, x)]
    peers.append(on_col(y, 1 - l, x))
    for peer in peers:
        pl.semaphore_signal(barrier, inc=1, device_id=peer, device_id_type=MESH)

    split_gu = one_hot((128, 128), lambda r: jnp.where(r < 64, 2 * r, 2 * r - 127))
    split_d = one_hot((64, 64), lambda r: jnp.where(r < 32, 2 * r, 2 * r - 63))
    mix_d = one_hot((128, 128), lambda r: (r & 3) * 32 + (r >> 2))
    mix_x = one_hot((256, 256), lambda r: (r & 3) * 64 + (r >> 2))

    def expand_gu(vals, meta, offset):
        def block(b, carry):
            for j in range(width // 128):
                at = slice(j * 128, (j + 1) * 128)
                v = vals[pl.ds(pl.multiple_of(b * 128, 128), 128), at]
                both = jnp.dot(split_gu, v, preferred_element_type=F32)
                codes = meta[pl.ds(pl.multiple_of(b * 64, 64), 64), at]
                for p, plane in enumerate(planes(both[:64], both[64:], codes)):
                    wgu[pl.ds(pl.multiple_of(b * 256 + p * 64, 64), 64), offset + j * 128 : offset + (j + 1) * 128] = plane.astype(BF16)
            return carry

        lax.fori_loop(0, vals.shape[0] // 128, block, 0)

    def expand_d(b, carry):
        for j in range(wd.shape[1] // 256):
            at = slice(j * 256, (j + 1) * 256)
            v = dv[pl.ds(pl.multiple_of(b * 64, 64), 64), at]
            both = jnp.dot(split_d, v, preferred_element_type=F32)
            codes = dm[pl.ds(pl.multiple_of(b * 32, 32), 32), at]
            for p, plane in enumerate(planes(both[:32], both[32:], codes)):
                wp[p * 32 : (p + 1) * 32, :] = plane.astype(BF16)
            dense = jnp.dot(mix_d, wp[...], preferred_element_type=F32)
            wd[pl.ds(pl.multiple_of(b * 128, 128), 128), at] = dense.astype(BF16)
        return carry

    loads[0].wait()
    loads[1].wait()
    expand_gu(gv, gm, 0)
    loads[4].wait()
    loads[5].wait()
    expand_gu(uv, um, width)
    loads[2].wait()
    loads[3].wait()

    def copy(src, dst, chunk, stage, to):
        return pltpu.make_async_remote_copy(
            src_ref=src, dst_ref=dst, send_sem=send.at[stage], recv_sem=recv.at[chunk, stage],
            device_id=to, device_id_type=MESH,
        )

    def arrive(dst, chunk, stage):
        copy(dst, dst, chunk, stage, partner).wait_recv()

    def ssq_copy(d):
        return pltpu.make_async_remote_copy(
            src_ref=ssq, dst_ref=ssq_in.at[d - 1], send_sem=ssq_sem.at[0], recv_sem=ssq_sem.at[1],
            device_id=((row + d) % 8, col), device_id_type=MESH,
        )

    def all_squares():
        return pltpu.make_async_remote_copy(
            src_ref=ssq_in, dst_ref=ssq_in, send_sem=ssq_sem.at[0], recv_sem=ssq_sem.at[1],
            device_id=partner, device_id_type=MESH,
        )

    def squares(i):
        def rows(n, carry):
            xf = tok[pl.ds(pl.multiple_of(n * ROWS, ROWS), ROWS), :].astype(F32)
            sums = jnp.sum(xf * xf, axis=1, keepdims=True)
            square = (ROWS, ROWS)
            diagonal = lax.broadcasted_iota(jnp.int32, square, 0) == lax.broadcasted_iota(jnp.int32, square, 1)
            ssq[pl.ds(n, 1), :] = jnp.sum(jnp.where(diagonal, sums, 0.0), axis=0, keepdims=True)
            return carry

        lax.fori_loop(0, CHUNKS, rows, 0)
        for d in range(1, 8):
            ssq_copy(d).start()

    order = step_order()
    first_chunk = [chunk for step, chunk in order if step == "product"][0]
    first_hidden = [chunk for step, chunk in order if step == "hidden"][0]

    def product(i):
        weighted = (tok[i * ROWS : (i + 2) * ROWS, :].astype(F32) * gain[...]).astype(BF16)
        for b in range(features // 256):
            at = slice(b * 256, (b + 1) * 256)
            xp[:, at] = jnp.dot(weighted[:, at], mix_x, preferred_element_type=F32).astype(BF16)
        for n in range(2 * width // 256):
            at = slice(n * 256, (n + 1) * 256)
            sums = jnp.dot(xp[...], wgu[:, at], preferred_element_type=F32).astype(BF16)
            part[i : i + 2, :, :, :, at] = sums.reshape(2, 2, 4, PIECE, 256)
        if i == first_chunk:
            pl.semaphore_wait(barrier, len(peers))
        for j in (i, i + 1):
            copy(part.at[j, 1 - c], pair_in.at[j], j, PAIR_IN, partner).start()

    def sums_of(w):
        return slice(w * width, (w + 1) * width)

    def paired(i, n, w):
        return part[i, c, n, :, sums_of(w)].astype(F32) + pair_in[i, n, :, sums_of(w)].astype(F32)

    def z_first(i):
        arrive(pair_in.at[i], i, PAIR_IN)
        for w in range(2):
            p1, _, other = z_of(w)
            s1[i, w, 0] = paired(i, p1, w).astype(BF16)
            s1[i, w, 1] = paired(i, other, w).astype(BF16)
            copy(s1.at[i, w], z1_in.at[i, w], i, Z_FIRST, to_z(p1)).start()

    def z_second(i):
        arrive(z1_in.at[i], i, Z_FIRST)
        for w in range(2):
            _, p2, _ = z_of(w)
            s2[i, w] = (paired(i, p2, w) + z1_in[i, w, 1].astype(F32)).astype(BF16)
            copy(s2.at[i, w], z2_in.at[i, w], i, Z_SECOND, to_z(p2)).start()

    def part_of(i, n, w):
        return hid.at[i, c, n, :, slice(0, 512) if w == 0 else slice(512, width)]

    def hidden(i):
        if i == first_hidden:
            all_squares().wait_recv()
            total = ssq[...]
            for d in range(1, 8):
                total = total + ssq_in[d - 1]
            scale[...] = lax.rsqrt(total / (features * 8) + EPS)
        lanes = (PIECE, ROWS)
        mine = c * 64 + k * PIECE + lax.broadcasted_iota(jnp.int32, lanes, 0)
        chosen = lax.broadcasted_iota(jnp.int32, lanes, 1) == mine
        factor = jnp.sum(jnp.where(chosen, scale[i : i + 1, :], 0.0), axis=1, keepdims=True)
        both = []
        arrive(z2_in.at[i], i, Z_SECOND)
        for w in range(2):
            both.append((paired(i, k, w) + z1_in[i, w, 0].astype(F32) + z2_in[i, w].astype(F32)) * factor)
        gate, up = both
        hid[i, c, k] = (gate / (1.0 + jnp.exp(-gate)) * up).astype(BF16)
        for w in range(2):
            mine = part_of(i, k, w)
            copy(mine, mine, i, Z_BACK, to_z(z_of(w)[1])).start()

    def z_last(i):
        arrive(hid.at[i, c, 0], i, Z_BACK)
        for w in range(2):
            p1, p2, _ = z_of(w)
            for mine in (part_of(i, k, w), part_of(i, p2, w)):
                copy(mine, mine, i, Z_LAST, to_z(p1)).start()

    def pair_out(i):
        arrive(hid.at[i, c, 0:2], i, Z_LAST)
        copy(hid.at[i, c], hid.at[i, c], i, PAIR_OUT, partner).start()

    def expand_down(i):
        loads[6].wait()
        loads[7].wait()
        lax.fori_loop(0, dv.shape[0] // 64, expand_d, 0)

    def down(i):
        arrive(hid.at[i, 1 - c], i, PAIR_OUT)
        for n in range(wd.shape[1] // 256):
            at = slice(n * 256, (n + 1) * 256)
            sums = jnp.dot(hid[i].reshape(ROWS, width), wd[:, at], preferred_element_type=F32).astype(BF16)
            dpart[i, :, :, :, at] = sums.reshape(2, 4, PIECE, 256)
        for v in range(2):
            for d in range(1, 4):
                src = dpart.at[i, v, (first_of(v) + d) % 4]
                copy(src, f_in.at[i, v, d - 1], i, F_OUT, first_peer(v, d)).start()

    def s_out(i):
        arrive(f_in.at[i], i, F_OUT)
        for v in range(2):
            total = dpart[i, v, first_of(v)].astype(F32)
            for d in range(1, 4):
                total = total + f_in[i, v, d - 1].astype(F32)
            total = total.astype(BF16)
            for q in range(4):
                s4[i, v, q] = total[:, q * 256 : (q + 1) * 256]
            for d in range(1, 4):
                src = s4.at[i, v, (second_of(v) + d) % 4]
                copy(src, s_in.at[i, v, d - 1], i, S_OUT, second_peer(v, d)).start()

    def between(i):
        arrive(s_in.at[i], i, S_OUT)
        for v in range(2):
            total = s4[i, v, second_of(v)].astype(F32)
            for d in range(1, 4):
                total = total + s_in[i, v, d - 1].astype(F32)
            s5[i, v] = total.astype(BF16)
        copy(s5.at[i], t_in.at[i], i, BETWEEN, opposite).start()

    def block_of(i, v, b):
        return out.at[i, v, first_of(v), :, pl.ds(pl.multiple_of(b * 256, 256), 256)]

    def s_back(i):
        arrive(t_in.at[i], i, BETWEEN)
        for v in range(2):
            rows = pl.ds(pl.multiple_of(i * ROWS + v * 64 + first_of(v) * PIECE, PIECE), PIECE)
            columns = pl.ds(pl.multiple_of(second_of(v) * 256, 256), 256)
            own = tok[rows, columns].astype(F32)
            result = own + (s5[i, v].astype(F32) + t_in[i, v].astype(F32))
            out[i, v, first_of(v), :, columns] = result.astype(BF16)
            mine = block_of(i, v, second_of(v))
            for d in range(1, 4):
                copy(mine, mine, i, S_BACK, second_peer(v, d)).start()

    def f_back(i):
        arrive(s_in.at[i], i, S_BACK)
        for v in range(2):
            mine = out.at[i, v, first_of(v)]
            for d in range(1, 4):
                copy(mine, mine, i, F_BACK, first_peer(v, d)).start()

    def arrived(i):
        arrive(f_in.at[i], i, F_BACK)

    bodies = dict(
        squares=squares, product=product, z_first=z_first, z_second=z_second, hidden=hidden, z_last=z_last, pair_out=pair_out,
        expand_down=expand_down, down=down, s_out=s_out, between=between, s_back=s_back, f_back=f_back, arrive=arrived,
    )
    for step, chunk in order:
        bodies[step](chunk)

    for stage, whole in (
        (PAIR_IN, pair_in), (Z_FIRST, z1_in), (Z_SECOND, z2_in), (Z_BACK, hid.at[:, 0, 0]), (Z_LAST, hid.at[:, 0, 0:2]),
        (PAIR_OUT, hid.at[:, 0]), (F_OUT, f_in), (S_OUT, s_in), (BETWEEN, t_in), (S_BACK, s_in), (F_BACK, f_in),
    ):
        copy(whole, whole, 0, stage, partner).wait_send()
    all_squares().wait_send()


def per_device(tokens, norm_gain, gate_vals, gate_meta, up_vals, up_meta, down_vals, down_meta):
    batch, features = tokens.shape
    width = gate_vals.shape[1]
    vmem = pltpu.VMEM
    scratch = [
        vmem(tokens.shape, BF16), vmem((1, features), F32),
        vmem(gate_vals.shape, BF16), vmem(gate_meta.shape, jnp.int32),
        vmem(up_vals.shape, BF16), vmem(up_meta.shape, jnp.int32),
        vmem(down_vals.shape, BF16), vmem(down_meta.shape, jnp.int32),
        vmem((features, 2 * width), BF16), vmem((width, features), BF16), vmem((128, 256), BF16), vmem((2 * ROWS, features), BF16),
        vmem((CHUNKS, 2, 4, PIECE, 2 * width), BF16), vmem((CHUNKS, 4, PIECE, 2 * width), BF16),
        vmem((CHUNKS, 2, 2, PIECE, width), BF16), vmem((CHUNKS, 2, 2, PIECE, width), BF16),
        vmem((CHUNKS, 2, PIECE, width), BF16), vmem((CHUNKS, 2, PIECE, width), BF16),
        vmem((CHUNKS, 2, 4, PIECE, width), BF16),
        vmem((CHUNKS, 2, 4, PIECE, features), BF16), vmem((CHUNKS, 2, 3, PIECE, features), BF16),
        vmem((CHUNKS, 2, 4, PIECE, 256), BF16), vmem((CHUNKS, 2, 3, PIECE, 256), BF16),
        vmem((CHUNKS, 2, PIECE, 256), BF16), vmem((CHUNKS, 2, PIECE, 256), BF16),
        vmem((CHUNKS, ROWS), F32), vmem((7, CHUNKS, ROWS), F32), vmem((CHUNKS, ROWS), F32),
        pltpu.SemaphoreType.DMA((8,)),
        pltpu.SemaphoreType.DMA((STAGES,)), pltpu.SemaphoreType.DMA((CHUNKS, STAGES)), pltpu.SemaphoreType.DMA((2,)),
    ]
    anywhere = pl.BlockSpec(memory_space=pl.ANY)
    out = pl.pallas_call(
        kernel,
        out_shape=pltpu.VMEM((CHUNKS, 2, 4, PIECE, features), BF16),
        in_specs=[anywhere] * 8,
        out_specs=pl.BlockSpec(memory_space=pltpu.VMEM),
        scratch_shapes=scratch,
        compiler_params=pltpu.CompilerParams(collective_id=0, has_side_effects=True, vmem_limit_bytes=60 * 1024 * 1024),
    )(tokens, norm_gain.reshape(1, features), gate_vals, gate_meta, up_vals, up_meta, down_vals, down_meta)
    return out.reshape(batch, features)


def solution(mesh):
    return jax.shard_map(
        per_device,
        mesh=mesh,
        in_specs=(
            P(None, "row"),
            P("row"),
            P("row", "col"),
            P("row", "col"),
            P("row", "col"),
            P("row", "col"),
            P("col", "row"),
            P("col", "row"),
        ),
        out_specs=P(None, "row"),
        check_vma=False,
    )
```

```python
import functools

import jax
import jax.numpy as jnp
from jax import lax
from jax.experimental import pallas as pl
from jax.experimental.pallas import tpu as pltpu
from jax.sharding import PartitionSpec as P

EPS = 1e-05
MESH = pl.DeviceIdType.MESH
F32 = jnp.float32
BF16 = jnp.bfloat16

CHUNKS = 8
ROWS = 128
PIECE = 16

PAIR_IN, Z_FIRST, Z_SECOND, Z_BACK, Z_LAST, PAIR_OUT, F_OUT, S_OUT, BETWEEN, S_BACK, F_BACK = range(11)
STAGES = 11

STEPS = (
    "squares", "expand_down", "product", "z_first", "z_second", "hidden", "z_last", "pair_out", "down", "s_out", "between", "s_back",
    "f_back", "arrive",
)
ORDER = (
    16, 24, 25, 22, 20, 30, 0, 32, 31, 18, 38, 27, 40, 39, 46, 28, 48, 47, 54, 26, 56, 35, 55, 33,
    62, 29, 8, 70, 34, 63, 43, 36, 64, 71, 41, 37, 78, 42, 51, 44, 49, 72, 79, 45, 50, 86, 59, 52,
    57, 67, 53, 58, 65, 60, 87, 94, 80, 66, 75, 61, 68, 73, 69, 95, 88, 74, 83, 102, 81, 76, 91, 77,
    103, 82, 89, 96, 110, 84, 90, 99, 85, 92, 111, 97, 93, 104, 98, 107, 100, 101, 105, 106, 108, 109,
)


def step_order():
    return [(STEPS[n // CHUNKS], n % CHUNKS) for n in ORDER]


def planes(first, second, meta):
    codes = meta.astype(F32).astype(BF16)
    none = jnp.zeros_like(first)
    low = codes < 3
    yield jnp.where(low, first, none)
    yield jnp.where(low, jnp.where(codes == 0, second, none), jnp.where(codes < 5, first, none))
    yield jnp.where((codes == 1) | (codes == 3), second, jnp.where(codes == 5, first, none))
    yield jnp.where((codes == 2) | (codes > 3), second, none)


def one_hot(shape, of_row):
    rows = lax.broadcasted_iota(jnp.int32, shape, 0)
    columns = lax.broadcasted_iota(jnp.int32, shape, 1)
    return jnp.where(columns == of_row(rows), 1.0, 0.0).astype(BF16)


def kernel(
    tok_h, gain_h, gv_h, gm_h, uv_h, um_h, dv_h, dm_h, out,
    tok, gain, gv, gm, uv, um, dv, dm, wgu, wd, wp, xp,
    part, pair_in, s1, z1_in, s2, z2_in, hid, dpart, f_in, s4, s_in, s5, t_in,
    ssq, ssq_in, scale,
    load_sem, block_sem, send, recv, ssq_sem,
):
    row = lax.axis_index("row")
    col = lax.axis_index("col")
    k, c = row // 2, row % 2
    y, l, x = col // 8, (col // 4) % 2, col % 4
    width = gv.shape[1]
    features = tok.shape[1]

    def on_row(k2, c2):
        return (k2 * 2 + c2, col)

    def on_col(y2, l2, x2):
        return (row, (y2 * 2 + l2) * 4 + x2)

    partner = on_row(k, 1 - c)

    def ways(n, way):
        near, far = n + 1 - 2 * (n % 2), 3 - n
        return (near, far) if way == 0 else (far, near)

    def z_of(way):
        p1, p2 = ways(k, way)
        return p1, p2, ways(p1, way)[1]

    def to_z(n):
        return on_row(n, c)

    def first_of(v):
        return x if v == 0 else y

    def second_of(v):
        return y if v == 0 else x

    def first_peer(v, d):
        if v == 0:
            return on_col(y, l, (x + d) % 4)
        return on_col((y + d) % 4, l, x)

    def second_peer(v, d):
        return first_peer(1 - v, d)

    opposite = on_col(y, 1 - l, x)

    def block_load(src, dst, n, b):
        rows = src.shape[0] // 4
        at = pl.ds(pl.multiple_of(b * rows, rows), rows)
        return pltpu.make_async_copy(src.at[at], dst.at[at], block_sem.at[n, b])

    blocks = ((gv_h, gv), (gm_h, gm), (uv_h, uv), (um_h, um))
    sources = (tok_h, gain_h, dv_h, dm_h)
    places = (tok, gain, dv, dm)
    loads = [pltpu.make_async_copy(a, b, load_sem.at[n]) for n, (a, b) in enumerate(zip(sources, places))]
    for n in range(2):
        for b in range(4):
            block_load(*blocks[2 * n], 2 * n, b).start()
            block_load(*blocks[2 * n + 1], 2 * n + 1, b).start()
    for load in loads:
        load.start()

    barrier = pltpu.get_barrier_semaphore()
    peers = [((row + d) % 8, col) for d in range(1, 8)]
    for d in range(1, 4):
        peers += [on_col(y, l, (x + d) % 4), on_col((y + d) % 4, l, x)]
    peers.append(on_col(y, 1 - l, x))
    for peer in peers:
        pl.semaphore_signal(barrier, inc=1, device_id=peer, device_id_type=MESH)

    split_gu = one_hot((128, 128), lambda r: jnp.where(r < 64, 2 * r, 2 * r - 127))
    split_d = one_hot((64, 64), lambda r: jnp.where(r < 32, 2 * r, 2 * r - 63))
    mix_d = one_hot((128, 128), lambda r: (r & 3) * 32 + (r >> 2))
    mix_x = one_hot((256, 256), lambda r: (r & 3) * 64 + (r >> 2))

    def expand_gu(vals, meta, offset, n):
        def block(b, carry):
            block_load(*blocks[n], n, b).wait()
            block_load(*blocks[n + 1], n + 1, b).wait()
            for j in range(width // 128):
                at = slice(j * 128, (j + 1) * 128)
                v = vals[pl.ds(pl.multiple_of(b * 128, 128), 128), at]
                both = jnp.dot(split_gu, v, preferred_element_type=F32).astype(BF16)
                codes = meta[pl.ds(pl.multiple_of(b * 64, 64), 64), at]
                for p, plane in enumerate(planes(both[:64], both[64:], codes)):
                    wgu[pl.ds(pl.multiple_of(b * 256 + p * 64, 64), 64), offset + j * 128 : offset + (j + 1) * 128] = plane
            return carry

        lax.fori_loop(0, 4, block, 0, unroll=True)

    def expand_d(b, carry):
        for j in range(wd.shape[1] // 256):
            at = slice(j * 256, (j + 1) * 256)
            v = dv[pl.ds(pl.multiple_of(b * 64, 64), 64), at]
            both = jnp.dot(split_d, v, preferred_element_type=F32).astype(BF16)
            codes = dm[pl.ds(pl.multiple_of(b * 32, 32), 32), at]
            for p, plane in enumerate(planes(both[:32], both[32:], codes)):
                wp[p * 32 : (p + 1) * 32, :] = plane
            dense = jnp.dot(mix_d, wp[...], preferred_element_type=F32)
            wd[pl.ds(pl.multiple_of(b * 128, 128), 128), at] = dense.astype(BF16)
        return carry

    expand_gu(gv, gm, 0, 0)
    expand_gu(uv, um, width, 2)
    loads[0].wait()
    loads[1].wait()

    def copy(src, dst, chunk, stage, to):
        return pltpu.make_async_remote_copy(
            src_ref=src, dst_ref=dst, send_sem=send.at[stage], recv_sem=recv.at[chunk, stage],
            device_id=to, device_id_type=MESH,
        )

    def arrive(dst, chunk, stage):
        copy(dst, dst, chunk, stage, partner).wait_recv()

    def ssq_copy(d):
        return pltpu.make_async_remote_copy(
            src_ref=ssq, dst_ref=ssq_in.at[d - 1], send_sem=ssq_sem.at[0], recv_sem=ssq_sem.at[1],
            device_id=((row + d) % 8, col), device_id_type=MESH,
        )

    def all_squares():
        return pltpu.make_async_remote_copy(
            src_ref=ssq_in, dst_ref=ssq_in, send_sem=ssq_sem.at[0], recv_sem=ssq_sem.at[1],
            device_id=partner, device_id_type=MESH,
        )

    def squares(i):
        def rows(n, carry):
            xf = tok[pl.ds(pl.multiple_of(n * ROWS, ROWS), ROWS), :].astype(F32)
            sums = jnp.sum(xf * xf, axis=1, keepdims=True)
            square = (ROWS, ROWS)
            diagonal = lax.broadcasted_iota(jnp.int32, square, 0) == lax.broadcasted_iota(jnp.int32, square, 1)
            ssq[pl.ds(n, 1), :] = jnp.sum(jnp.where(diagonal, sums, 0.0), axis=0, keepdims=True)
            return carry

        lax.fori_loop(0, CHUNKS, rows, 0)
        for d in range(1, 8):
            ssq_copy(d).start()

    order = step_order()
    first_chunk = [chunk for step, chunk in order if step == "product"][0]
    first_hidden = [chunk for step, chunk in order if step == "hidden"][0]

    def multiply(i, count):
        rows = slice(0, count * ROWS)
        weighted = (tok[i * ROWS : (i + count) * ROWS, :].astype(F32) * gain[...]).astype(BF16)
        for b in range(features // 256):
            at = slice(b * 256, (b + 1) * 256)
            xp[rows, at] = jnp.dot(weighted[:, at], mix_x, preferred_element_type=F32).astype(BF16)
        for n in range(2 * width // 256):
            at = slice(n * 256, (n + 1) * 256)
            sums = jnp.dot(xp[rows, :], wgu[:, at], preferred_element_type=F32).astype(BF16)
            part[i : i + count, :, :, :, at] = sums.reshape(count, 2, 4, PIECE, 256)

    def to_partner(i):
        copy(part.at[i, 1 - c], pair_in.at[i], i, PAIR_IN, partner).start()

    def product(i):
        if i == first_chunk:
            multiply(i, 1)
            pl.semaphore_wait(barrier, len(peers))
            to_partner(i)
            multiply(i + 1, 1)
        else:
            multiply(i, 2)
            to_partner(i)
        to_partner(i + 1)

    def sums_of(w):
        return slice(w * width, (w + 1) * width)

    def paired(i, n, w):
        return part[i, c, n, :, sums_of(w)].astype(F32) + pair_in[i, n, :, sums_of(w)].astype(F32)

    def z_first(i):
        arrive(pair_in.at[i], i, PAIR_IN)
        for w in range(2):
            p1, _, other = z_of(w)
            s1[i, w, 0] = paired(i, p1, w).astype(BF16)
            s1[i, w, 1] = paired(i, other, w).astype(BF16)
            copy(s1.at[i, w], z1_in.at[i, w], i, Z_FIRST, to_z(p1)).start()

    def z_second(i):
        arrive(z1_in.at[i], i, Z_FIRST)
        for w in range(2):
            _, p2, _ = z_of(w)
            s2[i, w] = (paired(i, p2, w) + z1_in[i, w, 1].astype(F32)).astype(BF16)
            copy(s2.at[i, w], z2_in.at[i, w], i, Z_SECOND, to_z(p2)).start()

    def part_of(i, n, w):
        return hid.at[i, c, n, :, slice(0, 512) if w == 0 else slice(512, width)]

    def hidden(i):
        if i == first_hidden:
            all_squares().wait_recv()
            total = ssq[...]
            for d in range(1, 8):
                total = total + ssq_in[d - 1]
            scale[...] = lax.rsqrt(total / (features * 8) + EPS)
        lanes = (PIECE, ROWS)
        mine = c * 64 + k * PIECE + lax.broadcasted_iota(jnp.int32, lanes, 0)
        chosen = lax.broadcasted_iota(jnp.int32, lanes, 1) == mine
        factor = jnp.sum(jnp.where(chosen, scale[i : i + 1, :], 0.0), axis=1, keepdims=True)
        both = []
        arrive(z2_in.at[i], i, Z_SECOND)
        for w in range(2):
            both.append((paired(i, k, w) + z1_in[i, w, 0].astype(F32) + z2_in[i, w].astype(F32)) * factor)
        gate, up = both
        hid[i, c, k] = (gate / (1.0 + jnp.exp(-gate)) * up).astype(BF16)
        for w in range(2):
            mine = part_of(i, k, w)
            copy(mine, mine, i, Z_BACK, to_z(z_of(w)[1])).start()

    def z_last(i):
        arrive(hid.at[i, c, 0], i, Z_BACK)
        for w in range(2):
            p1, p2, _ = z_of(w)
            for mine in (part_of(i, k, w), part_of(i, p2, w)):
                copy(mine, mine, i, Z_LAST, to_z(p1)).start()

    def pair_out(i):
        arrive(hid.at[i, c, 0:2], i, Z_LAST)
        copy(hid.at[i, c], hid.at[i, c], i, PAIR_OUT, partner).start()

    def expand_down(i):
        loads[2].wait()
        loads[3].wait()
        lax.fori_loop(0, dv.shape[0] // 64, expand_d, 0, unroll=True)

    def down(i):
        arrive(hid.at[i, 1 - c], i, PAIR_OUT)
        for n in range(wd.shape[1] // 256):
            at = slice(n * 256, (n + 1) * 256)
            sums = jnp.dot(hid[i].reshape(ROWS, width), wd[:, at], preferred_element_type=F32).astype(BF16)
            dpart[i, :, :, :, at] = sums.reshape(2, 4, PIECE, 256)
        for v in range(2):
            for d in range(1, 4):
                src = dpart.at[i, v, (first_of(v) + d) % 4]
                copy(src, f_in.at[i, v, d - 1], i, F_OUT, first_peer(v, d)).start()

    def s_out(i):
        arrive(f_in.at[i], i, F_OUT)
        for v in range(2):
            total = dpart[i, v, first_of(v)].astype(F32)
            for d in range(1, 4):
                total = total + f_in[i, v, d - 1].astype(F32)
            total = total.astype(BF16)
            for q in range(4):
                s4[i, v, q] = total[:, q * 256 : (q + 1) * 256]
            for d in range(1, 4):
                src = s4.at[i, v, (second_of(v) + d) % 4]
                copy(src, s_in.at[i, v, d - 1], i, S_OUT, second_peer(v, d)).start()

    def between(i):
        arrive(s_in.at[i], i, S_OUT)
        for v in range(2):
            total = s4[i, v, second_of(v)].astype(F32)
            for d in range(1, 4):
                total = total + s_in[i, v, d - 1].astype(F32)
            s5[i, v] = total.astype(BF16)
        copy(s5.at[i], t_in.at[i], i, BETWEEN, opposite).start()

    def block_of(i, v, b):
        return out.at[i, v, first_of(v), :, pl.ds(pl.multiple_of(b * 256, 256), 256)]

    def s_back(i):
        arrive(t_in.at[i], i, BETWEEN)
        for v in range(2):
            rows = pl.ds(pl.multiple_of(i * ROWS + v * 64 + first_of(v) * PIECE, PIECE), PIECE)
            columns = pl.ds(pl.multiple_of(second_of(v) * 256, 256), 256)
            own = tok[rows, columns].astype(F32)
            result = own + (s5[i, v].astype(F32) + t_in[i, v].astype(F32))
            out[i, v, first_of(v), :, columns] = result.astype(BF16)
            mine = block_of(i, v, second_of(v))
            for d in range(1, 4):
                copy(mine, mine, i, S_BACK, second_peer(v, d)).start()

    def f_back(i):
        arrive(s_in.at[i], i, S_BACK)
        for v in range(2):
            mine = out.at[i, v, first_of(v)]
            for d in range(1, 4):
                copy(mine, mine, i, F_BACK, first_peer(v, d)).start()

    def arrived(i):
        arrive(f_in.at[i], i, F_BACK)

    bodies = dict(
        squares=squares, product=product, z_first=z_first, z_second=z_second, hidden=hidden, z_last=z_last, pair_out=pair_out,
        expand_down=expand_down, down=down, s_out=s_out, between=between, s_back=s_back, f_back=f_back, arrive=arrived,
    )
    for step, chunk in order:
        bodies[step](chunk)

    for stage, whole in (
        (PAIR_IN, pair_in), (Z_FIRST, z1_in), (Z_SECOND, z2_in), (Z_BACK, hid.at[:, 0, 0]), (Z_LAST, hid.at[:, 0, 0:2]),
        (PAIR_OUT, hid.at[:, 0]), (F_OUT, f_in), (S_OUT, s_in), (BETWEEN, t_in), (S_BACK, s_in), (F_BACK, f_in),
    ):
        copy(whole, whole, 0, stage, partner).wait_send()
    all_squares().wait_send()


def per_device(tokens, norm_gain, gate_vals, gate_meta, up_vals, up_meta, down_vals, down_meta):
    batch, features = tokens.shape
    width = gate_vals.shape[1]
    vmem = pltpu.VMEM
    scratch = [
        vmem(tokens.shape, BF16), vmem((1, features), F32),
        vmem(gate_vals.shape, BF16), vmem(gate_meta.shape, jnp.int32),
        vmem(up_vals.shape, BF16), vmem(up_meta.shape, jnp.int32),
        vmem(down_vals.shape, BF16), vmem(down_meta.shape, jnp.int32),
        vmem((features, 2 * width), BF16), vmem((width, features), BF16), vmem((128, 256), BF16), vmem((2 * ROWS, features), BF16),
        vmem((CHUNKS, 2, 4, PIECE, 2 * width), BF16), vmem((CHUNKS, 4, PIECE, 2 * width), BF16),
        vmem((CHUNKS, 2, 2, PIECE, width), BF16), vmem((CHUNKS, 2, 2, PIECE, width), BF16),
        vmem((CHUNKS, 2, PIECE, width), BF16), vmem((CHUNKS, 2, PIECE, width), BF16),
        vmem((CHUNKS, 2, 4, PIECE, width), BF16),
        vmem((CHUNKS, 2, 4, PIECE, features), BF16), vmem((CHUNKS, 2, 3, PIECE, features), BF16),
        vmem((CHUNKS, 2, 4, PIECE, 256), BF16), vmem((CHUNKS, 2, 3, PIECE, 256), BF16),
        vmem((CHUNKS, 2, PIECE, 256), BF16), vmem((CHUNKS, 2, PIECE, 256), BF16),
        vmem((CHUNKS, ROWS), F32), vmem((7, CHUNKS, ROWS), F32), vmem((CHUNKS, ROWS), F32),
        pltpu.SemaphoreType.DMA((4,)), pltpu.SemaphoreType.DMA((4, 4)),
        pltpu.SemaphoreType.DMA((STAGES,)), pltpu.SemaphoreType.DMA((CHUNKS, STAGES)), pltpu.SemaphoreType.DMA((2,)),
    ]
    anywhere = pl.BlockSpec(memory_space=pl.ANY)
    out = pl.pallas_call(
        kernel,
        out_shape=pltpu.VMEM((CHUNKS, 2, 4, PIECE, features), BF16),
        in_specs=[anywhere] * 8,
        out_specs=pl.BlockSpec(memory_space=pltpu.VMEM),
        scratch_shapes=scratch,
        compiler_params=pltpu.CompilerParams(collective_id=0, has_side_effects=True, vmem_limit_bytes=60 * 1024 * 1024),
    )(tokens, norm_gain.reshape(1, features), gate_vals, gate_meta, up_vals, up_meta, down_vals, down_meta)
    return out.reshape(batch, features)


def solution(mesh):
    return jax.shard_map(
        per_device,
        mesh=mesh,
        in_specs=(
            P(None, "row"),
            P("row"),
            P("row", "col"),
            P("row", "col"),
            P("row", "col"),
            P("row", "col"),
            P("col", "row"),
            P("col", "row"),
        ),
        out_specs=P(None, "row"),
        check_vma=False,
    )
```

```python
import functools

import jax
import jax.numpy as jnp
from jax import lax
from jax.experimental import pallas as pl
from jax.experimental.pallas import tpu as pltpu
from jax.sharding import PartitionSpec as P

EPS = 1e-05
MESH = pl.DeviceIdType.MESH
F32 = jnp.float32
BF16 = jnp.bfloat16

CHUNKS = 8
ROWS = 128
PIECE = 16

PAIR_IN, Z_FIRST, Z_SECOND, Z_BACK, Z_LAST, PAIR_OUT, F_OUT, S_OUT, BETWEEN, S_BACK, F_BACK, PAIR_GATE, PAIR_UP = range(13)
STAGES = 13

STEPS = (
    "squares", "expand_down", "product", "z_first", "z_second", "hidden", "z_last", "pair_out", "down", "s_out", "between", "s_back",
    "f_back", "arrive",
)
FAR_FIRST = (2, 1, 3)

ORDER = (
    16, 24, 20, 25, 22, 29, 0, 32, 33, 31, 18, 37, 41, 40, 27, 39, 49, 48, 45, 26, 35, 57, 30, 47,
    56, 28, 34, 53, 8, 65, 38, 64, 43, 36, 42, 55, 61, 73, 46, 51, 69, 44, 50, 81, 63, 72, 54, 71,
    59, 52, 77, 58, 89, 67, 62, 66, 80, 79, 60, 70, 85, 68, 75, 93, 74, 87, 88, 78, 97, 76, 83, 95,
    101, 82, 86, 91, 96, 105, 84, 90, 94, 103, 109, 92, 99, 104, 98, 102, 111, 100, 107, 106, 110, 108,
)


def step_order():
    return [(STEPS[n // CHUNKS], n % CHUNKS) for n in ORDER]


def planes(first, second, meta):
    codes = meta.astype(F32).astype(BF16)
    none = jnp.zeros_like(first)
    low = codes < 3
    yield jnp.where(low, first, none)
    yield jnp.where(low, jnp.where(codes == 0, second, none), jnp.where(codes < 5, first, none))
    yield jnp.where((codes == 1) | (codes == 3), second, jnp.where(codes == 5, first, none))
    yield jnp.where((codes == 2) | (codes > 3), second, none)


def one_hot(shape, of_row):
    rows = lax.broadcasted_iota(jnp.int32, shape, 0)
    columns = lax.broadcasted_iota(jnp.int32, shape, 1)
    return jnp.where(columns == of_row(rows), 1.0, 0.0).astype(BF16)


def kernel(
    tok_h, gain_h, gv_h, gm_h, uv_h, um_h, dv_h, dm_h, out,
    tok, gain, gv, gm, uv, um, dv, dm, wgu, wd, wp, xp,
    part, pair_in, s1, z1_in, s2, z2_in, hid, dpart, f_in, s4, s_in, s5, t_in,
    ssq, ssq_in, scale,
    load_sem, block_sem, send, recv, ssq_sem,
):
    row = lax.axis_index("row")
    col = lax.axis_index("col")
    k, c = row // 2, row % 2
    y, l, x = col // 8, (col // 4) % 2, col % 4
    width = gv.shape[1]
    features = tok.shape[1]

    def on_row(k2, c2):
        return (k2 * 2 + c2, col)

    def on_col(y2, l2, x2):
        return (row, (y2 * 2 + l2) * 4 + x2)

    partner = on_row(k, 1 - c)

    def ways(n, way):
        near, far = n + 1 - 2 * (n % 2), 3 - n
        return (near, far) if way == 0 else (far, near)

    def z_of(way):
        p1, p2 = ways(k, way)
        return p1, p2, ways(p1, way)[1]

    def to_z(n):
        return on_row(n, c)

    def first_of(v):
        return x if v == 0 else y

    def second_of(v):
        return y if v == 0 else x

    def first_peer(v, d):
        if v == 0:
            return on_col(y, l, (x + d) % 4)
        return on_col((y + d) % 4, l, x)

    def second_peer(v, d):
        return first_peer(1 - v, d)

    opposite = on_col(y, 1 - l, x)

    def block_load(src, dst, n, b):
        rows = src.shape[0] // 4
        at = pl.ds(pl.multiple_of(b * rows, rows), rows)
        return pltpu.make_async_copy(src.at[at], dst.at[at], block_sem.at[n, b])

    blocks = ((gv_h, gv), (gm_h, gm), (uv_h, uv), (um_h, um))
    sources = (tok_h, gain_h, dv_h, dm_h)
    places = (tok, gain, dv, dm)
    loads = [pltpu.make_async_copy(a, b, load_sem.at[n]) for n, (a, b) in enumerate(zip(sources, places))]
    for n in range(2):
        for b in range(4):
            block_load(*blocks[2 * n], 2 * n, b).start()
            block_load(*blocks[2 * n + 1], 2 * n + 1, b).start()
        loads[2 * n].start()
        loads[2 * n + 1].start()

    barrier = pltpu.get_barrier_semaphore()
    peers = [((row + d) % 8, col) for d in range(1, 8)]
    for d in range(1, 4):
        peers += [on_col(y, l, (x + d) % 4), on_col((y + d) % 4, l, x)]
    peers.append(on_col(y, 1 - l, x))
    for peer in peers:
        pl.semaphore_signal(barrier, inc=1, device_id=peer, device_id_type=MESH)

    split_gu = one_hot((128, 128), lambda r: jnp.where(r < 64, 2 * r, 2 * r - 127))
    split_d = one_hot((64, 64), lambda r: jnp.where(r < 32, 2 * r, 2 * r - 63))
    mix_d = one_hot((128, 128), lambda r: (r & 3) * 32 + (r >> 2))
    mix_x = one_hot((256, 256), lambda r: (r & 3) * 64 + (r >> 2))

    def expand_gu(vals, meta, offset, n):
        def block(b, carry):
            block_load(*blocks[n], n, b).wait()
            block_load(*blocks[n + 1], n + 1, b).wait()
            for start in range(0, width, 256):
                at = slice(start, min(start + 256, width))
                v = vals[pl.ds(pl.multiple_of(b * 128, 128), 128), at]
                both = jnp.dot(split_gu, v, preferred_element_type=F32).astype(BF16)
                codes = meta[pl.ds(pl.multiple_of(b * 64, 64), 64), at]
                for p, plane in enumerate(planes(both[:64], both[64:], codes)):
                    wgu[pl.ds(pl.multiple_of(b * 256 + p * 64, 64), 64), offset + at.start : offset + at.stop] = plane
            return carry

        lax.fori_loop(0, 4, block, 0, unroll=True)

    def expand_d(b, carry):
        for j in range(wd.shape[1] // 256):
            at = slice(j * 256, (j + 1) * 256)
            v = dv[pl.ds(pl.multiple_of(b * 64, 64), 64), at]
            both = jnp.dot(split_d, v, preferred_element_type=F32).astype(BF16)
            codes = dm[pl.ds(pl.multiple_of(b * 32, 32), 32), at]
            for p, plane in enumerate(planes(both[:32], both[32:], codes)):
                wp[p * 32 : (p + 1) * 32, :] = plane
            dense = jnp.dot(mix_d, wp[...], preferred_element_type=F32)
            wd[pl.ds(pl.multiple_of(b * 128, 128), 128), at] = dense.astype(BF16)
        return carry


    def copy(src, dst, chunk, stage, to):
        return pltpu.make_async_remote_copy(
            src_ref=src, dst_ref=dst, send_sem=send.at[stage], recv_sem=recv.at[chunk, stage],
            device_id=to, device_id_type=MESH,
        )

    def arrive(dst, chunk, stage):
        copy(dst, dst, chunk, stage, partner).wait_recv()

    def ssq_copy(d):
        return pltpu.make_async_remote_copy(
            src_ref=ssq, dst_ref=ssq_in.at[d - 1], send_sem=ssq_sem.at[0], recv_sem=ssq_sem.at[1],
            device_id=((row + d) % 8, col), device_id_type=MESH,
        )

    def all_squares():
        return pltpu.make_async_remote_copy(
            src_ref=ssq_in, dst_ref=ssq_in, send_sem=ssq_sem.at[0], recv_sem=ssq_sem.at[1],
            device_id=partner, device_id_type=MESH,
        )

    def squares(i):
        def rows(n, carry):
            xf = tok[pl.ds(pl.multiple_of(n * ROWS, ROWS), ROWS), :].astype(F32)
            sums = jnp.sum(xf * xf, axis=1, keepdims=True)
            square = (ROWS, ROWS)
            diagonal = lax.broadcasted_iota(jnp.int32, square, 0) == lax.broadcasted_iota(jnp.int32, square, 1)
            ssq[pl.ds(n, 1), :] = jnp.sum(jnp.where(diagonal, sums, 0.0), axis=0, keepdims=True)
            return carry

        lax.fori_loop(0, CHUNKS, rows, 0)
        for d in range(1, 8):
            ssq_copy(d).start()

    order = step_order()
    first_chunk = [chunk for step, chunk in order if step == "product"][0]
    first_hidden = [chunk for step, chunk in order if step == "hidden"][0]

    def bring_together(i, count):
        weighted = (tok[i * ROWS : (i + count) * ROWS, :].astype(F32) * gain[...]).astype(BF16)
        for b in range(features // 256):
            at = slice(b * 256, (b + 1) * 256)
            xp[0 : count * ROWS, at] = jnp.dot(weighted[:, at], mix_x, preferred_element_type=F32).astype(BF16)

    def multiply(i, count, first, last):
        for start in range(first, last, 256):
            at = slice(start, min(start + 256, last))
            sums = jnp.dot(xp[0 : count * ROWS, :], wgu[:, at], preferred_element_type=F32).astype(BF16)
            part[i : i + count, :, :, :, at] = sums.reshape(count, 2, 4, PIECE, at.stop - at.start)

    def to_partner(i):
        copy(part.at[i, 1 - c], pair_in.at[i], i, PAIR_IN, partner).start()

    def product(i):
        if i == first_chunk:
            bring_together(i + 1, 1)
            multiply(i + 1, 1, 0, 2 * width)
        else:
            bring_together(i, 2)
            multiply(i, 2, 0, 2 * width)
            to_partner(i)
        to_partner(i + 1)

    def sums_of(w):
        return slice(w * width, (w + 1) * width)

    def paired(i, n, w):
        return part[i, c, n, :, sums_of(w)].astype(F32) + pair_in[i, n, :, sums_of(w)].astype(F32)

    def z_first_of(i, w):
        p1, _, other = z_of(w)
        s1[i, w, 0] = paired(i, p1, w).astype(BF16)
        s1[i, w, 1] = paired(i, other, w).astype(BF16)
        copy(s1.at[i, w], z1_in.at[i, w], i, Z_FIRST, to_z(p1)).start()

    def z_first(i):
        if i == first_chunk:
            arrive(pair_in.at[i, :, :, sums_of(1)], i, PAIR_UP)
            z_first_of(i, 1)
        else:
            arrive(pair_in.at[i], i, PAIR_IN)
            z_first_of(i, 0)
            z_first_of(i, 1)

    def half_to_partner(i, w, stage):
        copy(part.at[i, 1 - c, :, :, sums_of(w)], pair_in.at[i, :, :, sums_of(w)], i, stage, partner).start()

    def begin(i):
        expand_gu(gv, gm, 0, 0)
        loads[0].wait()
        loads[1].wait()
        bring_together(i, 1)
        multiply(i, 1, 0, width)
        pl.semaphore_wait(barrier, len(peers))
        half_to_partner(i, 0, PAIR_GATE)
        expand_gu(uv, um, width, 2)
        arrive(pair_in.at[i, :, :, sums_of(0)], i, PAIR_GATE)
        z_first_of(i, 0)
        multiply(i, 1, width, 2 * width)
        half_to_partner(i, 1, PAIR_UP)

    def z_second(i):
        arrive(z1_in.at[i], i, Z_FIRST)
        for w in range(2):
            _, p2, _ = z_of(w)
            s2[i, w] = (paired(i, p2, w) + z1_in[i, w, 1].astype(F32)).astype(BF16)
            copy(s2.at[i, w], z2_in.at[i, w], i, Z_SECOND, to_z(p2)).start()

    def part_of(i, n, w):
        return hid.at[i, c, n, :, slice(0, 512) if w == 0 else slice(512, width)]

    def hidden(i):
        if i == first_hidden:
            all_squares().wait_recv()
            total = ssq[...]
            for d in range(1, 8):
                total = total + ssq_in[d - 1]
            scale[...] = lax.rsqrt(total / (features * 8) + EPS)
        lanes = (PIECE, ROWS)
        mine = c * 64 + k * PIECE + lax.broadcasted_iota(jnp.int32, lanes, 0)
        chosen = lax.broadcasted_iota(jnp.int32, lanes, 1) == mine
        factor = jnp.sum(jnp.where(chosen, scale[i : i + 1, :], 0.0), axis=1, keepdims=True)
        both = []
        arrive(z2_in.at[i], i, Z_SECOND)
        for w in range(2):
            both.append((paired(i, k, w) + z1_in[i, w, 0].astype(F32) + z2_in[i, w].astype(F32)) * factor)
        gate, up = both
        hid[i, c, k] = (gate / (1.0 + jnp.exp(-gate)) * up).astype(BF16)
        for w in range(2):
            mine = part_of(i, k, w)
            copy(mine, mine, i, Z_BACK, to_z(z_of(w)[1])).start()

    def z_last(i):
        arrive(hid.at[i, c, 0], i, Z_BACK)
        for w in range(2):
            p1, p2, _ = z_of(w)
            for mine in (part_of(i, k, w), part_of(i, p2, w)):
                copy(mine, mine, i, Z_LAST, to_z(p1)).start()

    def pair_out(i):
        arrive(hid.at[i, c, 0:2], i, Z_LAST)
        copy(hid.at[i, c], hid.at[i, c], i, PAIR_OUT, partner).start()

    def expand_down(i):
        loads[2].wait()
        loads[3].wait()
        lax.fori_loop(0, dv.shape[0] // 64, expand_d, 0, unroll=True)

    def down(i):
        arrive(hid.at[i, 1 - c], i, PAIR_OUT)
        for n in range(wd.shape[1] // 256):
            at = slice(n * 256, (n + 1) * 256)
            sums = jnp.dot(hid[i].reshape(ROWS, width), wd[:, at], preferred_element_type=F32).astype(BF16)
            dpart[i, :, :, :, at] = sums.reshape(2, 4, PIECE, 256)
        for v in range(2):
            for d in FAR_FIRST:
                src = dpart.at[i, v, (first_of(v) + d) % 4]
                copy(src, f_in.at[i, v, d - 1], i, F_OUT, first_peer(v, d)).start()

    def s_out(i):
        arrive(f_in.at[i], i, F_OUT)
        for v in range(2):
            total = dpart[i, v, first_of(v)].astype(F32)
            for d in range(1, 4):
                total = total + f_in[i, v, d - 1].astype(F32)
            total = total.astype(BF16)
            for q in range(4):
                s4[i, v, q] = total[:, q * 256 : (q + 1) * 256]
            for d in FAR_FIRST:
                src = s4.at[i, v, (second_of(v) + d) % 4]
                copy(src, s_in.at[i, v, d - 1], i, S_OUT, second_peer(v, d)).start()

    def between(i):
        arrive(s_in.at[i], i, S_OUT)
        for v in range(2):
            total = s4[i, v, second_of(v)].astype(F32)
            for d in range(1, 4):
                total = total + s_in[i, v, d - 1].astype(F32)
            s5[i, v] = total.astype(BF16)
        copy(s5.at[i], t_in.at[i], i, BETWEEN, opposite).start()

    def block_of(i, v, b):
        return out.at[i, v, first_of(v), :, pl.ds(pl.multiple_of(b * 256, 256), 256)]

    def s_back(i):
        arrive(t_in.at[i], i, BETWEEN)
        for v in range(2):
            rows = pl.ds(pl.multiple_of(i * ROWS + v * 64 + first_of(v) * PIECE, PIECE), PIECE)
            columns = pl.ds(pl.multiple_of(second_of(v) * 256, 256), 256)
            own = tok[rows, columns].astype(F32)
            result = own + (s5[i, v].astype(F32) + t_in[i, v].astype(F32))
            out[i, v, first_of(v), :, columns] = result.astype(BF16)
            mine = block_of(i, v, second_of(v))
            for d in FAR_FIRST:
                copy(mine, mine, i, S_BACK, second_peer(v, d)).start()

    def f_back(i):
        arrive(s_in.at[i], i, S_BACK)
        for v in range(2):
            mine = out.at[i, v, first_of(v)]
            for d in FAR_FIRST:
                copy(mine, mine, i, F_BACK, first_peer(v, d)).start()

    def arrived(i):
        arrive(f_in.at[i], i, F_BACK)

    bodies = dict(
        squares=squares, product=product, z_first=z_first, z_second=z_second, hidden=hidden, z_last=z_last, pair_out=pair_out,
        expand_down=expand_down, down=down, s_out=s_out, between=between, s_back=s_back, f_back=f_back, arrive=arrived,
    )
    begin(first_chunk)
    for step, chunk in order:
        bodies[step](chunk)

    for stage, whole in (
        (PAIR_GATE, pair_in.at[0, :, :, sums_of(0)]), (PAIR_UP, pair_in.at[0, :, :, sums_of(1)]), (PAIR_IN, pair_in.at[1:]),
        (Z_FIRST, z1_in), (Z_SECOND, z2_in), (Z_BACK, hid.at[:, 0, 0]), (Z_LAST, hid.at[:, 0, 0:2]),
        (PAIR_OUT, hid.at[:, 0]), (F_OUT, f_in), (S_OUT, s_in), (BETWEEN, t_in), (S_BACK, s_in), (F_BACK, f_in),
    ):
        copy(whole, whole, 0, stage, partner).wait_send()
    all_squares().wait_send()


def per_device(tokens, norm_gain, gate_vals, gate_meta, up_vals, up_meta, down_vals, down_meta):
    batch, features = tokens.shape
    width = gate_vals.shape[1]
    vmem = pltpu.VMEM
    scratch = [
        vmem(tokens.shape, BF16), vmem((1, features), F32),
        vmem(gate_vals.shape, BF16), vmem(gate_meta.shape, jnp.int32),
        vmem(up_vals.shape, BF16), vmem(up_meta.shape, jnp.int32),
        vmem(down_vals.shape, BF16), vmem(down_meta.shape, jnp.int32),
        vmem((features, 2 * width), BF16), vmem((width, features), BF16), vmem((128, 256), BF16), vmem((2 * ROWS, features), BF16),
        vmem((CHUNKS, 2, 4, PIECE, 2 * width), BF16), vmem((CHUNKS, 4, PIECE, 2 * width), BF16),
        vmem((CHUNKS, 2, 2, PIECE, width), BF16), vmem((CHUNKS, 2, 2, PIECE, width), BF16),
        vmem((CHUNKS, 2, PIECE, width), BF16), vmem((CHUNKS, 2, PIECE, width), BF16),
        vmem((CHUNKS, 2, 4, PIECE, width), BF16),
        vmem((CHUNKS, 2, 4, PIECE, features), BF16), vmem((CHUNKS, 2, 3, PIECE, features), BF16),
        vmem((CHUNKS, 2, 4, PIECE, 256), BF16), vmem((CHUNKS, 2, 3, PIECE, 256), BF16),
        vmem((CHUNKS, 2, PIECE, 256), BF16), vmem((CHUNKS, 2, PIECE, 256), BF16),
        vmem((CHUNKS, ROWS), F32), vmem((7, CHUNKS, ROWS), F32), vmem((CHUNKS, ROWS), F32),
        pltpu.SemaphoreType.DMA((4,)), pltpu.SemaphoreType.DMA((4, 4)),
        pltpu.SemaphoreType.DMA((STAGES,)), pltpu.SemaphoreType.DMA((CHUNKS, STAGES)), pltpu.SemaphoreType.DMA((2,)),
    ]
    anywhere = pl.BlockSpec(memory_space=pl.ANY)
    out = pl.pallas_call(
        kernel,
        out_shape=pltpu.VMEM((CHUNKS, 2, 4, PIECE, features), BF16),
        in_specs=[anywhere] * 8,
        out_specs=pl.BlockSpec(memory_space=pltpu.VMEM),
        scratch_shapes=scratch,
        compiler_params=pltpu.CompilerParams(collective_id=0, has_side_effects=True, vmem_limit_bytes=60 * 1024 * 1024),
    )(tokens, norm_gain.reshape(1, features), gate_vals, gate_meta, up_vals, up_meta, down_vals, down_meta)
    return out.reshape(batch, features)


def solution(mesh):
    return jax.shard_map(
        per_device,
        mesh=mesh,
        in_specs=(
            P(None, "row"),
            P("row"),
            P("row", "col"),
            P("row", "col"),
            P("row", "col"),
            P("row", "col"),
            P("col", "row"),
            P("col", "row"),
        ),
        out_specs=P(None, "row"),
        check_vma=False,
    )
```
